1024 devices in a mesh: lat: 64 (over x, y), lev: 16 (over z, core).
Axes of the slice: x: 8, y: 8, z: 8, core: 2. Of those that a mesh axis runs over, the one named last changes fastest.
Arguments:
- fourier: bfloat16 [256, 2560, 128], P('lev', 'lat'), may hold values from -6 to 6
- quad_weights: float32 [2560], P('lat'), may hold values from 0.005 to 0.05
- legendre: bfloat16 [2560, 64, 1280], P('lat'), may hold values from -6 to 6
- owner_pair: int32 [64], replicated, may hold values from 0 to 63, each once
Outputs:
- spectra: float32 [64, 256, 1280], P('lat', 'lev')
- energy: float32 [], replicated
The draws below stay inside these ranges and needn't reach their ends.
Inputs may be any that keep to these rules, and one draw needn't show every extreme that they name: `owner_pair`: a permutation of 0 to 63.
All inputs are finite; a program needn't handle non-finite values.
Results may differ from the reference program's by a relative error of at most 0.00094.
Values may be sent and summed in bfloat16 or wider, within the bound.
A program may use at most 64 MiB of HBM per device.

```python
import math
import jax
import jax.numpy as jnp
from jax import lax

TRUNC = 1280
NLAT = 2560
M_WIN = 128
SPACING = 10
LEVELS = 128
CHANNELS = 256
NPAIR = 64
PAIRLEN = 1280


def draw_fourier(key, part):
    base = jax.random.fold_in(key, 11)
    rough_key, common_key = jax.random.split(base)
    common_normal = jnp.clip(jax.random.normal(common_key, (CHANNELS, 1, M_WIN), jnp.float32), -4.0, 4.0)
    rough = jnp.clip(jax.random.normal(rough_key, (CHANNELS, NLAT, M_WIN), jnp.float32), -4.0, 4.0)
    common = 0.3 * common_normal
    return (rough + common).astype(jnp.bfloat16)


def draw_legendre(key, part):
    base = jax.random.fold_in(key, 23)
    rough_key, mask_key, sign_key, pairing_key = jax.random.split(base, 4)
    pairing = jax.random.permutation(pairing_key, NPAIR).astype(jnp.int32)
    group = jnp.arange(NLAT, dtype=jnp.int32) * NPAIR // NLAT
    paired = group[:, None, None] == pairing[None, :, None]
    amplitude = jnp.where(paired, 3.0, 1.0)
    rough = jnp.clip(jax.random.normal(rough_key, (NLAT, NPAIR, PAIRLEN), jnp.float32), -4.0, 4.0)
    spike_size = 2.0
    diffuse = jnp.clip(amplitude * rough, -6.0, 6.0)
    chosen = jax.random.randint(mask_key, (NPAIR, PAIRLEN), 0, 64) == 0
    signs = (2 * jax.random.randint(sign_key, (NPAIR, PAIRLEN), 0, 2) - 1).astype(jnp.float32)
    spiked = signs[None, :, :] * spike_size + 0.25 * rough
    return jnp.where(chosen[None, :, :], spiked, diffuse).astype(jnp.bfloat16)


def steps_of(stream_key, dims, pieces, least, top_value):
    loudness = 1.0
    for position, blocks in pieces:
        draws = jax.random.uniform(jax.random.fold_in(jax.random.fold_in(stream_key, 6), position), (blocks,), jnp.float32, least / len(pieces), top_value / len(pieces))
        loudness = loudness * jnp.repeat(jnp.exp(draws), dims[position] // blocks).reshape((-1,) + (1,) * (len(dims) - 1 - position))
    return loudness


def setup_inputs(seed: int = 0) -> dict:
    streams_of = jax.random.split(jax.random.key(seed), 5)
    fourier = draw_fourier(jax.random.fold_in(streams_of[4], 71), 0)
    quad_weights = jnp.clip(jnp.exp(math.log(0.05) - 2.3025851 * jax.random.uniform(streams_of[1], (NLAT,), jnp.float32) ** steps_of(streams_of[1], (NLAT,), ((0, 64),), -0.2, 0.2)), 0.005, 0.05)
    legendre = draw_legendre(jax.random.fold_in(streams_of[4], 71), 0)
    owner_pair = jax.random.permutation(streams_of[3], NPAIR).astype(jnp.int32)
    return dict(fourier=fourier, quad_weights=quad_weights, legendre=legendre, owner_pair=owner_pair)


def reference(fourier, quad_weights, legendre, owner_pair):
    weighted = (fourier.astype(jnp.float32) * quad_weights[None, :, None]).astype(jnp.bfloat16)
    column_ids = jnp.arange(PAIRLEN, dtype=jnp.int32)

    def one_pair(pair_id):
        legendre_part = legendre[:, pair_id, :]
        low_wave = weighted[:, :, pair_id]
        high_wave = weighted[:, :, M_WIN - 1 - pair_id]
        low_part = jnp.dot(low_wave, legendre_part, preferred_element_type=jnp.float32)
        high_part = jnp.dot(high_wave, legendre_part, preferred_element_type=jnp.float32)
        low_limit = TRUNC - SPACING * pair_id - SPACING // 2
        return jnp.where(column_ids[None, :] < low_limit, low_part, high_part)

    spectra = lax.map(one_pair, owner_pair)
    channel_ids = jnp.arange(2 * LEVELS, dtype=jnp.int32)
    level_factor = 1.0 + 2.0 * (channel_ids // 2).astype(jnp.float32) / (LEVELS - 1)
    energy = jnp.sum(level_factor[None, :, None] * spectra * spectra) / (NPAIR * 2 * LEVELS * PAIRLEN)
    return (spectra, energy)
```

```python
import functools

import jax
import jax.numpy as jnp
import numpy as np
from jax import lax
from jax.experimental import pallas as pl
from jax.experimental.pallas import tpu as pltpu
from jax.sharding import Mesh
from jax.sharding import PartitionSpec as P

MESH = pl.DeviceIdType.MESH
TRUNC = 1280
M_WIN = 128
SPACING = 10
LAT = ("lat_0", "lat_1")
LEV = ("lev_0", "lev_1")
LANE = 128
SUB = 5
GROUPS = ((0, 3), (3, 5), (5, 7))
TABLE_GROUPS = (0, 1)
WAVE_GROUP = 2


def row_orders(n):
    rows = n * n * SUB
    r = np.arange(rows)
    b, src, l = r // (n * SUB), r // SUB % n, r % SUB
    q1 = np.zeros((rows, rows), np.float32)
    q1[r, src * n * SUB + l * n + b] = 1
    q2 = np.zeros((rows, rows), np.float32)
    q2[r, src * n * SUB + b * SUB + l] = 1
    return q1, q2


def kernel(n, nz, f_hbm, w_smem, leg_hbm, pair_row_hbm, pair_smem, q1_hbm, q2_hbm, out_ref, energy_ref,
           f_in, f_rows, tin, pair_row, q1, q2, z_send, z_recv, p1s, p1r, p2s, p2r, w_sib,
           part, a3, a4, merged, fin, fin_sib, e0, e1, e2,
           load_sem, zs_sem, zr_sem, p1s_sem, p1r_sem, p2s_sem, p2r_sem, w_sem,
           a_ssem, a_rsem, n_ssem, n_rsem, m_ssem, f_sem, e_ssem, e_rsem):
    x, y, z, c = (lax.axis_index(a) for a in LAT + LEV)
    ch = f_in.shape[0]
    half = tin.shape[2]
    chunks = half // LANE
    other = 1 - c
    pairs = n * n

    def core_xy(first, j):
        along_x = (c == 0) if first else (c == 1)
        return (jnp.where(along_x, j, x), jnp.where(along_x, y, j), z, c)

    me_first = jnp.where(c == 0, x, y)
    me_second = jnp.where(c == 0, y, x)

    def wrap(v, size):
        return lax.rem(v + size, size)

    barrier = pltpu.get_barrier_semaphore()
    count = 0
    for r in range(1, n):
        pl.semaphore_signal(barrier, inc=1, device_id=(wrap(x + r, n), y, z, c), device_id_type=MESH)
        pl.semaphore_signal(barrier, inc=1, device_id=(x, wrap(y + r, n), z, c), device_id_type=MESH)
        count += 2
    for r in range(1, nz):
        pl.semaphore_signal(barrier, inc=1, device_id=(x, y, wrap(z + r, nz), c), device_id_type=MESH)
        pl.semaphore_signal(barrier, inc=1, device_id=(x, y, wrap(z + r, nz), other), device_id_type=MESH)
        count += 2
    pl.semaphore_signal(barrier, inc=1, device_id=(x, y, z, other), device_id_type=MESH)
    count += 1

    loads = [
        pltpu.make_async_copy(f_hbm, f_in, load_sem.at[0]),
        pltpu.make_async_copy(
            leg_hbm.at[pl.ds(SUB * z, SUB), :, pl.ds(pl.multiple_of(c * half, LANE), half)], tin, load_sem.at[1]
        ),
        pltpu.make_async_copy(pair_row_hbm, pair_row, load_sem.at[2]),
        pltpu.make_async_copy(q1_hbm, q1, load_sem.at[3]),
        pltpu.make_async_copy(q2_hbm, q2, load_sem.at[4]),
    ]
    for load in loads:
        load.start()

    def remote(src, dst, ssem, rsem, device):
        return pltpu.make_async_remote_copy(
            src_ref=src, dst_ref=dst, send_sem=ssem, recv_sem=rsem, device_id=device, device_id_type=MESH
        )

    loads[0].wait()
    lats = f_in.shape[1]
    f_rows[...] = f_in[...].astype(jnp.float32).reshape(ch * lats, M_WIN)
    for l in range(lats):
        z_send[l // SUB, l % SUB] = f_rows[pl.ds(l, ch, stride=lats), :].astype(jnp.bfloat16)
    z_recv[z] = z_send[z]

    loads[2].wait()
    row_i = lax.broadcasted_iota(jnp.int32, (pairs, pairs), 0)
    col_i = lax.broadcasted_iota(jnp.int32, (pairs, pairs), 1)
    owner_of_col = jnp.where(c == 0, col_i, lax.rem(col_i, n) * n + lax.div(col_i, n))
    order = jnp.where(row_i == owner_of_col, 1.0, 0.0).astype(jnp.bfloat16)
    wave_i = lax.broadcasted_iota(jnp.int32, (M_WIN, pairs), 0)
    ids = jnp.broadcast_to(pair_row[0:1, 0:pairs], (M_WIN, pairs))
    low_hot = jnp.where(wave_i == ids, 1.0, 0.0).astype(jnp.bfloat16)
    high_hot = jnp.where(M_WIN - 1 - wave_i == ids, 1.0, 0.0).astype(jnp.bfloat16)

    def nt(a, b):
        return lax.dot_general(a, b, (((1,), (1,)), ((), ())), preferred_element_type=jnp.float32)

    low_sel = nt(order, low_hot).astype(jnp.bfloat16)
    high_sel = nt(order, high_hot).astype(jnp.bfloat16)

    pl.semaphore_wait(barrier, count)

    far_first = [r for k in range(n // 2, 0, -1) for r in sorted({k, n - k})]
    z_far_first = [r for k in range(nz // 2, 0, -1) for r in sorted({k, nz - k})]
    for r in z_far_first:
        t = wrap(z + r, nz)
        remote(z_send.at[t], z_recv.at[z], zs_sem, zr_sem, (x, y, t, c)).start()

    def send_first(g):
        j0, j1 = GROUPS[g]
        p1r[j0:j1, me_first] = p1s[j0:j1, me_first]
        for r in far_first:
            t = wrap(me_first + r, n)
            remote(
                p1s.at[j0:j1, t], p1r.at[j0:j1, me_first], p1s_sem.at[g], p1r_sem.at[g], core_xy(True, t)
            ).start()

    def forward(g):
        j0, j1 = GROUPS[g]
        if n > 1:
            got = p1r.at[j0:j1, 0 : n - 1]
            remote(got, got, p1s_sem.at[g], p1r_sem.at[g], core_xy(True, me_first)).wait_recv()
        for j in range(j0, j1):
            rows = p1r[j].reshape(n * SUB * n, LANE)
            p2s[j] = jnp.dot(q1[...], rows, preferred_element_type=jnp.float32).astype(jnp.bfloat16).reshape(p2s.shape[1:])
        p2r[j0:j1, me_second] = p2s[j0:j1, me_second]
        for r in far_first:
            t = wrap(me_second + r, n)
            remote(
                p2s.at[j0:j1, t], p2r.at[j0:j1, me_second], p2s_sem.at[g], p2r_sem.at[g], core_xy(False, t)
            ).start()

    def received_second(g):
        j0, j1 = GROUPS[g]
        if n > 1:
            got = p2r.at[j0:j1, 0 : n - 1]
            remote(got, got, p2s_sem.at[g], p2r_sem.at[g], core_xy(False, me_second)).wait_recv()

    loads[1].wait()
    table_sel = low_sel[:, 0:pairs]
    for g in TABLE_GROUPS:
        j0, j1 = GROUPS[g]
        for l in range(SUB):
            rows = jnp.dot(table_sel, tin[l, :, j0 * LANE : j1 * LANE], preferred_element_type=jnp.float32)
            rows = rows.astype(jnp.bfloat16)
            for j in range(j0, j1):
                at = (j - j0) * LANE
                p1s[j, :, l] = rows[:, at : at + LANE].reshape(n, n, LANE)
        send_first(g)

    loads[3].wait()
    loads[4].wait()
    forward(0)

    if nz > 1:
        got = z_recv.at[0 : nz - 1]
        remote(got, got, zs_sem, zr_sem, (x, y, z, c)).wait_recv()
    for l in range(SUB):
        block = z_recv[:, l].reshape(nz * ch, M_WIN)
        weight = w_smem[SUB * z + l]
        p1s[chunks, :, l] = (nt(low_sel, block) * weight).astype(jnp.bfloat16).reshape(n, n, LANE)
        p1s[chunks + 1, :, l] = (nt(high_sel, block) * weight).astype(jnp.bfloat16).reshape(n, n, LANE)
    send_first(WAVE_GROUP)
    forward(1)
    forward(WAVE_GROUP)

    received_second(WAVE_GROUP)
    swap = remote(p2r.at[chunks : chunks + 2], w_sib, w_sem.at[0], w_sem.at[1], (x, y, z, other))
    swap.start()
    for g in TABLE_GROUPS:
        received_second(g)
    rows_of = n * n * SUB
    mine = [p2r[chunks + i].reshape(rows_of, LANE) for i in range(2)]
    swap.wait_recv()
    theirs = [
        jnp.dot(q2[...], w_sib[i].reshape(rows_of, LANE), preferred_element_type=jnp.float32).astype(jnp.bfloat16)
        for i in range(2)
    ]
    waves = jnp.concatenate([mine[0], theirs[0], mine[1], theirs[1]], axis=1)

    limit = TRUNC - SPACING * pair_smem[x * n + y] - SPACING // 2
    for j in range(chunks):
        table = p2r[j].reshape(rows_of, LANE)
        both = lax.dot_general(waves, table, (((0,), (0,)), ((), ())), preferred_element_type=jnp.float32)
        column = c * half + j * LANE + lax.broadcasted_iota(jnp.int32, (2 * LANE, LANE), 1)
        sums = jnp.where(column < limit, both[: 2 * LANE], both[2 * LANE :])
        part[:, :, :, j * LANE : (j + 1) * LANE] = sums.reshape(2, nz, ch, LANE)

    sends = []
    if nz > 1:
        def up(k):
            return wrap(z + k + nz, nz)

        for i, sign in enumerate((1, -1)):
            sends.append(remote(part.at[:, up(3 * sign)], a3.at[i], a_ssem.at[i], a_rsem.at[i], (x, y, up(sign), c)))
            sends.append(remote(part.at[i, up(4)], a4.at[i], a_ssem.at[2 + i], a_rsem.at[2 + i], (x, y, up(2 * sign), c)))
        for i, sign in enumerate((1, -1)):
            for h in range(2):
                to = (x, y, up(sign), jnp.where(h == 0, c, other))
                sends.append(remote(part.at[h, up(sign)], fin.at[h, i], n_ssem.at[h, i], n_rsem.at[h, i], to))
    own = remote(part.at[1, z], fin_sib, f_sem.at[0], f_sem.at[1], (x, y, z, other))
    for send in sends:
        send.start()
    own.start()
    if nz > 1:
        late = []
        for i, sign in enumerate((1, -1)):
            remote(a3.at[i], a3.at[i], a_ssem.at[i], a_rsem.at[i], (x, y, z, c)).wait_recv()
            remote(a4.at[i], a4.at[i], a_ssem.at[2 + i], a_rsem.at[2 + i], (x, y, z, c)).wait_recv()
            merged[i] = part[:, up(2 * sign)] + a3[i]
            merged[i, i] = merged[i, i] + a4[i]
            for h in range(2):
                to = (x, y, up(2 * sign), jnp.where(h == 0, c, other))
                send = remote(merged.at[i, h], fin.at[h, 2 + i], m_ssem.at[h, i], n_rsem.at[h, 2 + i], to)
                send.start()
                late.append(send)
        sends = sends + late
    own.wait_recv()
    total = [part[0, z], fin_sib[...]]
    if nz > 1:
        for i in range(4):
            for h in range(2):
                remote(fin.at[h, i], fin.at[h, i], f_sem.at[0], n_rsem.at[h, i], (x, y, z, c)).wait_recv()
                total[h] = total[h] + fin[h, i]

    out_ref[:, pl.ds(pl.multiple_of(c * half, LANE), half)] = total[0]
    out_ref[:, pl.ds(pl.multiple_of(other * half, LANE), half)] = total[1]
    levels = nz * 2 * ch // 2
    channel = (z * 2 + c) * ch + lax.broadcasted_iota(jnp.int32, (ch, half), 0)
    factor = 1.0 + 2.0 * lax.shift_right_logical(channel, 1).astype(jnp.float32) / (levels - 1)
    squares = factor * (total[0] * total[0] + total[1] * total[1])
    tile = jnp.zeros((8, LANE), jnp.float32)
    for i in range(ch // 8):
        for j in range(chunks):
            tile = tile + squares[i * 8 : i * 8 + 8, j * LANE : (j + 1) * LANE]

    def added(ref, size, at, tile, sem, devices):
        ref[at] = tile
        for device in devices:
            remote(ref.at[at], ref.at[at], e_ssem.at[sem], e_rsem.at[sem], device).start()
        if size > 1:
            got = ref.at[0 : size - 1]
            remote(got, got, e_ssem.at[sem], e_rsem.at[sem], (x, y, z, c)).wait_recv()
        tile = ref[0]
        for i in range(1, size):
            tile = tile + ref[i]
        return tile

    peers = [(x, y, wrap(z + r, nz), k) for r in z_far_first for k in (c, other)] + [(x, y, z, other)]
    tile = added(e0, nz * 2, z * 2 + c, tile, 0, peers)
    tile = added(e1, n, y, tile, 1, [(x, wrap(y + r, n), z, c) for r in far_first])
    tile = added(e2, n, x, tile, 2, [(wrap(x + r, n), y, z, c) for r in far_first])
    energy_ref[0, 0] = jnp.sum(tile) / (pairs * 2 * levels * 2 * half)

    if nz > 1:
        gone = z_send.at[0 : nz - 1]
        remote(gone, gone, zs_sem, zr_sem, (x, y, z, c)).wait_send()
    if n > 1:
        for g, (j0, j1) in enumerate(GROUPS):
            gone = p1s.at[j0:j1, 0 : n - 1]
            remote(gone, gone, p1s_sem.at[g], p1r_sem.at[g], (x, y, z, c)).wait_send()
            gone = p2s.at[j0:j1, 0 : n - 1]
            remote(gone, gone, p2s_sem.at[g], p2r_sem.at[g], (x, y, z, c)).wait_send()
    swap.wait_send()
    own.wait_send()
    for send in sends:
        send.wait_send()
    for sem, ref, size in ((0, e0, nz * 2), (1, e1, n), (2, e2, n)):
        if size > 1:
            gone = ref.at[0 : size - 1]
            remote(gone, gone, e_ssem.at[sem], e_rsem.at[sem], (x, y, z, c)).wait_send()


def shards(n, nz, fourier, quad_weights, legendre, owner_pair):
    ch, lats, _ = fourier.shape
    _, pairs, length = legendre.shape
    half = length // 2
    chunks = half // LANE
    rows = n * n * SUB
    q1, q2 = row_orders(n)
    pair_row = jnp.pad(owner_pair, (0, LANE - pairs)).reshape(1, LANE)
    bf16, f32 = jnp.bfloat16, jnp.float32
    vmem, dma = pltpu.VMEM, pltpu.SemaphoreType.DMA
    any_space = pl.BlockSpec(memory_space=pl.ANY)
    smem = pl.BlockSpec(memory_space=pltpu.SMEM)
    exchange = (chunks + 2, n, SUB, n, LANE)
    spectra, energy = pl.pallas_call(
        functools.partial(kernel, n, nz),
        out_shape=(
            jax.ShapeDtypeStruct((ch, length), f32),
            jax.ShapeDtypeStruct((1, 1), f32),
        ),
        in_specs=[any_space, smem, any_space, any_space, smem, any_space, any_space],
        out_specs=(pl.BlockSpec(memory_space=pltpu.VMEM), smem),
        scratch_shapes=[
            vmem((ch, lats, M_WIN), bf16),
            vmem((ch * lats, M_WIN), f32),
            vmem((SUB, pairs, half), bf16),
            vmem((1, LANE), jnp.int32),
            vmem((rows, rows), bf16),
            vmem((rows, rows), bf16),
            vmem((nz, SUB, ch, M_WIN), bf16),
            vmem((nz, SUB, ch, M_WIN), bf16),
            vmem(exchange, bf16),
            vmem(exchange, bf16),
            vmem(exchange, bf16),
            vmem(exchange, bf16),
            vmem((2, *exchange[1:]), bf16),
            vmem((2, nz, ch, half), f32),
            vmem((2, 2, ch, half), f32),
            vmem((2, ch, half), f32),
            vmem((2, 2, ch, half), f32),
            vmem((2, 4, ch, half), f32),
            vmem((ch, half), f32),
            vmem((nz * 2, 8, LANE), f32),
            vmem((n, 8, LANE), f32),
            vmem((n, 8, LANE), f32),
            dma((5,)),
            dma,
            dma,
            dma((3,)),
            dma((3,)),
            dma((3,)),
            dma((3,)),
            dma((2,)),
            dma((4,)),
            dma((4,)),
            dma((2, 2)),
            dma((2, 4)),
            dma((2, 2)),
            dma((2,)),
            dma((3,)),
            dma((3,)),
        ],
        compiler_params=pltpu.CompilerParams(
            collective_id=0, has_side_effects=True, vmem_limit_bytes=40 * 1024 * 1024
        ),
        name="legendre",
    )(fourier, quad_weights, legendre, pair_row, owner_pair, jnp.asarray(q1, bf16), jnp.asarray(q2, bf16))
    return spectra[None], energy[0, 0]


def solution(mesh):
    n = round(mesh.shape["lat"] ** 0.5)
    nz = mesh.shape["lev"] // 2
    finer = Mesh(mesh.devices.reshape(n, n, nz, 2), LAT + LEV)
    return jax.shard_map(
        functools.partial(shards, n, nz),
        mesh=finer,
        in_specs=(P(LEV, LAT, None), P(LAT), P(LAT, None, None), P()),
        out_specs=(P(LAT, LEV, None), P()),
        check_vma=False,
    )
```

```python
import functools

import jax
import jax.numpy as jnp
import numpy as np
from jax import lax
from jax.experimental import pallas as pl
from jax.experimental.pallas import tpu as pltpu
from jax.sharding import Mesh
from jax.sharding import PartitionSpec as P

MESH = pl.DeviceIdType.MESH
TRUNC = 1280
M_WIN = 128
SPACING = 10
LAT = ("lat_0", "lat_1")
LEV = ("lev_0", "lev_1")
LANE = 128
SUB = 5
GROUPS = ((0, 1), (1, 3), (3, 5), (5, 7))
TABLE_GROUPS = (0, 1, 2)
WAVE_GROUP = 3
EARLY = (0,)
LATE = (1, 2)


def row_orders(n):
    rows = n * n * SUB
    r = np.arange(rows)
    b, src, l = r // (n * SUB), r // SUB % n, r % SUB
    q1 = np.zeros((rows, rows), np.float32)
    q1[r, src * n * SUB + l * n + b] = 1
    q2 = np.zeros((rows, rows), np.float32)
    q2[r, src * n * SUB + b * SUB + l] = 1
    return q1, q2


def kernel(n, nz, f_hbm, w_hbm, leg_hbm, pair_row_hbm, pair_hbm, q1_hbm, q2_hbm, out_hbm, energy_ref,
           f_in, f_rows, tin, pair_row, pair_smem, w_smem, q1, q2, z_send, z_recv, p1s, p1r, p2s, p2r, t_sib,
           t_perm, part, a3, a4, merged, fin, out_buf, e0, e1, e2,
           load_sem, zs_sem, zr_sem, p1s_sem, p1r_sem, p2s_sem, p2r_sem, t_ssem, t_rsem,
           a_ssem, a_rsem, f_ssem, f_rsem, e_ssem, e_rsem):
    x, y, z, c = (lax.axis_index(a) for a in LAT + LEV)
    ch = f_in.shape[0]
    half = tin.shape[2]
    chunks = half // LANE
    other = 1 - c
    pairs = n * n
    rows_of = n * n * SUB

    def core_xy(first, j):
        along_x = (c == 0) if first else (c == 1)
        return (jnp.where(along_x, j, x), jnp.where(along_x, y, j), z, c)

    me_first = jnp.where(c == 0, x, y)
    me_second = jnp.where(c == 0, y, x)

    def wrap(v, size):
        return lax.rem(v + size, size)

    loads = [
        pltpu.make_async_copy(f_hbm, f_in, load_sem.at[0]),
        pltpu.make_async_copy(pair_row_hbm, pair_row, load_sem.at[2]),
        pltpu.make_async_copy(
            leg_hbm.at[pl.ds(SUB * z, SUB), :, pl.ds(pl.multiple_of(c * half, LANE), half)], tin, load_sem.at[1]
        ),
        pltpu.make_async_copy(q1_hbm, q1, load_sem.at[3]),
        pltpu.make_async_copy(w_hbm, w_smem, load_sem.at[5]),
        pltpu.make_async_copy(pair_hbm, pair_smem, load_sem.at[6]),
        pltpu.make_async_copy(q2_hbm, q2, load_sem.at[4]),
    ]
    for load in loads:
        load.start()
    f_load, pair_row_load, table_load, q1_load, w_load, pair_load, q2_load = loads

    barrier = pltpu.get_barrier_semaphore()
    count = 0
    for r in range(1, n):
        pl.semaphore_signal(barrier, inc=1, device_id=(wrap(x + r, n), y, z, c), device_id_type=MESH)
        pl.semaphore_signal(barrier, inc=1, device_id=(x, wrap(y + r, n), z, c), device_id_type=MESH)
        count += 2
    for r in range(1, nz):
        pl.semaphore_signal(barrier, inc=1, device_id=(x, y, wrap(z + r, nz), c), device_id_type=MESH)
        pl.semaphore_signal(barrier, inc=1, device_id=(x, y, wrap(z + r, nz), other), device_id_type=MESH)
        count += 2
    pl.semaphore_signal(barrier, inc=1, device_id=(x, y, z, other), device_id_type=MESH)
    count += 1

    def remote(src, dst, ssem, rsem, device):
        return pltpu.make_async_remote_copy(
            src_ref=src, dst_ref=dst, send_sem=ssem, recv_sem=rsem, device_id=device, device_id_type=MESH
        )

    f_load.wait()
    lats = f_in.shape[1]
    f_rows[...] = f_in[...].astype(jnp.float32).reshape(ch * lats, M_WIN)
    for l in range(lats):
        z_send[l // SUB, l % SUB] = f_rows[pl.ds(l, ch, stride=lats), :].astype(jnp.bfloat16)
    z_recv[z] = z_send[z]

    pl.semaphore_wait(barrier, count)

    far_first = [r for k in range(n // 2, 0, -1) for r in sorted({k, n - k})]
    z_far_first = [r for k in range(nz // 2, 0, -1) for r in sorted({k, nz - k})]
    for r in z_far_first:
        t = wrap(z + r, nz)
        remote(z_send.at[t], z_recv.at[z], zs_sem, zr_sem, (x, y, t, c)).start()

    pair_row_load.wait()
    row_i = lax.broadcasted_iota(jnp.int32, (pairs, pairs), 0)
    col_i = lax.broadcasted_iota(jnp.int32, (pairs, pairs), 1)
    owner_of_col = jnp.where(c == 0, col_i, lax.rem(col_i, n) * n + lax.div(col_i, n))
    order = jnp.where(row_i == owner_of_col, 1.0, 0.0).astype(jnp.bfloat16)
    wave_i = lax.broadcasted_iota(jnp.int32, (M_WIN, pairs), 0)
    ids = jnp.broadcast_to(pair_row[...], (M_WIN, pairs))
    low_hot = jnp.where(wave_i == ids, 1.0, 0.0).astype(jnp.bfloat16)
    high_hot = jnp.where(M_WIN - 1 - wave_i == ids, 1.0, 0.0).astype(jnp.bfloat16)

    def nt(a, b):
        return lax.dot_general(a, b, (((1,), (1,)), ((), ())), preferred_element_type=jnp.float32)

    low_sel = nt(order, low_hot).astype(jnp.bfloat16)
    high_sel = nt(order, high_hot).astype(jnp.bfloat16)

    def send_first(g):
        j0, j1 = GROUPS[g]
        p1r[j0:j1, me_first] = p1s[j0:j1, me_first]
        for r in far_first:
            t = wrap(me_first + r, n)
            remote(
                p1s.at[j0:j1, t], p1r.at[j0:j1, me_first], p1s_sem.at[g], p1r_sem.at[g], core_xy(True, t)
            ).start()

    def forward(g):
        j0, j1 = GROUPS[g]
        if n > 1:
            got = p1r.at[j0:j1, 0 : n - 1]
            remote(got, got, p1s_sem.at[g], p1r_sem.at[g], core_xy(True, me_first)).wait_recv()
        for j in range(j0, j1):
            rows = p1r[j].reshape(rows_of, LANE)
            p2s[j] = jnp.dot(q1[...], rows, preferred_element_type=jnp.float32).astype(jnp.bfloat16).reshape(p2s.shape[1:])
        p2r[j0:j1, me_second] = p2s[j0:j1, me_second]
        for r in far_first:
            t = wrap(me_second + r, n)
            remote(
                p2s.at[j0:j1, t], p2r.at[j0:j1, me_second], p2s_sem.at[g], p2r_sem.at[g], core_xy(False, t)
            ).start()

    def received_second(g):
        j0, j1 = GROUPS[g]
        if n > 1:
            got = p2r.at[j0:j1, 0 : n - 1]
            remote(got, got, p2s_sem.at[g], p2r_sem.at[g], core_xy(False, me_second)).wait_recv()

    table_load.wait()
    table_sel = low_sel[:, 0:pairs]
    for g in TABLE_GROUPS:
        j0, j1 = GROUPS[g]
        for l in range(SUB):
            rows = jnp.dot(table_sel, tin[l, :, j0 * LANE : j1 * LANE], preferred_element_type=jnp.float32)
            rows = rows.astype(jnp.bfloat16)
            for j in range(j0, j1):
                at = (j - j0) * LANE
                p1s[j, :, l] = rows[:, at : at + LANE].reshape(n, n, LANE)
        send_first(g)

    for load in (q1_load, w_load, pair_load, q2_load):
        load.wait()
    for g in EARLY:
        forward(g)

    if nz > 1:
        got = z_recv.at[0 : nz - 1]
        remote(got, got, zs_sem, zr_sem, (x, y, z, c)).wait_recv()
    for l in range(SUB):
        block = z_recv[:, l].reshape(nz * ch, M_WIN)
        weight = w_smem[SUB * z + l]
        p1s[chunks, :, l] = (nt(low_sel, block) * weight).astype(jnp.bfloat16).reshape(n, n, LANE)
        p1s[chunks + 1, :, l] = (nt(high_sel, block) * weight).astype(jnp.bfloat16).reshape(n, n, LANE)
    send_first(WAVE_GROUP)
    for g in LATE:
        forward(g)
    forward(WAVE_GROUP)

    swaps = []
    for g in TABLE_GROUPS:
        received_second(g)
        j0, j1 = GROUPS[g]
        swap = remote(p2r.at[j0:j1], t_sib.at[j0:j1], t_ssem.at[g], t_rsem.at[g], (x, y, z, other))
        swap.start()
        swaps.append(swap)
    for g in TABLE_GROUPS:
        swaps[g].wait_recv()
        for j in range(*GROUPS[g]):
            rows = t_sib[j].reshape(rows_of, LANE)
            t_perm[j] = jnp.dot(q2[...], rows, preferred_element_type=jnp.float32).astype(jnp.bfloat16)

    received_second(WAVE_GROUP)
    waves = jnp.concatenate([p2r[chunks + i].reshape(rows_of, LANE) for i in range(2)], axis=1)
    limit = TRUNC - SPACING * pair_smem[x * n + y] - SPACING // 2
    for j in range(0, 2 * chunks, 2):
        blocks = [p2r[i].reshape(rows_of, LANE) if i < chunks else t_perm[i - chunks] for i in (j, j + 1)]
        table = jnp.concatenate(blocks, axis=1)
        both = lax.dot_general(waves, table, (((0,), (0,)), ((), ())), preferred_element_type=jnp.float32)
        for i in range(2):
            first = c * half + (j + i) * LANE if j + i < chunks else other * half + (j + i - chunks) * LANE
            column = first + lax.broadcasted_iota(jnp.int32, (LANE, LANE), 1)
            at = i * LANE
            sums = jnp.where(column < limit, both[:LANE, at : at + LANE], both[LANE:, at : at + LANE])
            part[:, :, (j + i) * LANE : (j + i + 1) * LANE] = sums.reshape(nz, ch, LANE)

    def up(k):
        return wrap(z + k + nz, nz)

    ways = ((0, 1), (1, -1)) if nz > 1 else ()
    sends = []
    for i, sign in ways:
        sends.append(remote(part.at[up(3 * sign)], a3.at[i], a_ssem.at[i], a_rsem.at[i], (x, y, up(sign), c)))
        sends.append(remote(
            part.at[up(4), :, i * half : (i + 1) * half], a4.at[i], a_ssem.at[2 + i], a_rsem.at[2 + i],
            (x, y, up(2 * sign), c),
        ))
    for i, sign in ways:
        sends.append(remote(part.at[up(sign)], fin.at[i], f_ssem.at[i], f_rsem.at[i], (x, y, up(sign), c)))
    for send in sends:
        send.start()
    for i, sign in ways:
        sends[2 * i].wait_recv()
        merged[i] = part[up(2 * sign)] + a3[i]
        sends[2 * i + 1].wait_recv()
        merged[i, :, i * half : (i + 1) * half] = merged[i, :, i * half : (i + 1) * half] + a4[i]
        send = remote(merged.at[i], fin.at[2 + i], f_ssem.at[2 + i], f_rsem.at[2 + i], (x, y, up(2 * sign), c))
        send.start()
        sends.append(send)
    total = part[z]
    for send in sends[4:]:
        send.wait_recv()
    for i in range(4 if nz > 1 else 0):
        total = total + fin[i]

    levels = nz * 2 * ch // 2
    channel = (z * 2 + c) * ch + lax.broadcasted_iota(jnp.int32, (ch, LANE), 0)
    factor = 1.0 + 2.0 * lax.shift_right_logical(channel, 1).astype(jnp.float32) / (levels - 1)
    columns = [total[:, j * LANE : (j + 1) * LANE] for j in range(2 * chunks)]
    squares = columns[0] * columns[0]
    for column in columns[1:]:
        squares = squares + column * column
    squares = factor * squares
    tile = squares[0:8]
    for i in range(1, ch // 8):
        tile = tile + squares[i * 8 : i * 8 + 8]

    def share(ref, at, tile, sem, devices):
        ref[at] = tile
        for device in devices:
            remote(ref.at[at], ref.at[at], e_ssem.at[sem], e_rsem.at[sem], device).start()

    def added(ref, size, sem):
        if size > 1:
            got = ref.at[0 : size - 1]
            remote(got, got, e_ssem.at[sem], e_rsem.at[sem], (x, y, z, c)).wait_recv()
        tile = ref[0]
        for i in range(1, size):
            tile = tile + ref[i]
        return tile

    peers = [(x, y, wrap(z + r, nz), k) for r in z_far_first for k in (c, other)] + [(x, y, z, other)]
    share(e0, z * 2 + c, tile, 0, peers)
    out_buf[:, pl.ds(pl.multiple_of(c * half, LANE), half)] = total[:, :half]
    out_buf[:, pl.ds(pl.multiple_of(other * half, LANE), half)] = total[:, half:]
    out_copy = pltpu.make_async_copy(out_buf, out_hbm, load_sem.at[7])
    out_copy.start()
    tile = added(e0, nz * 2, 0)
    share(e1, y, tile, 1, [(x, wrap(y + r, n), z, c) for r in far_first])
    tile = added(e1, n, 1)
    share(e2, x, tile, 2, [(wrap(x + r, n), y, z, c) for r in far_first])
    tile = added(e2, n, 2)
    energy_ref[0, 0] = jnp.sum(tile) / (pairs * 2 * levels * 2 * half)

    out_copy.wait()
    if nz > 1:
        gone = z_send.at[0 : nz - 1]
        remote(gone, gone, zs_sem, zr_sem, (x, y, z, c)).wait_send()
    if n > 1:
        for g, (j0, j1) in enumerate(GROUPS):
            gone = p1s.at[j0:j1, 0 : n - 1]
            remote(gone, gone, p1s_sem.at[g], p1r_sem.at[g], (x, y, z, c)).wait_send()
            gone = p2s.at[j0:j1, 0 : n - 1]
            remote(gone, gone, p2s_sem.at[g], p2r_sem.at[g], (x, y, z, c)).wait_send()
    for send in swaps + sends:
        send.wait_send()
    for sem, ref, size in ((0, e0, nz * 2), (1, e1, n), (2, e2, n)):
        if size > 1:
            gone = ref.at[0 : size - 1]
            remote(gone, gone, e_ssem.at[sem], e_rsem.at[sem], (x, y, z, c)).wait_send()


def shards(n, nz, fourier, quad_weights, legendre, owner_pair):
    ch, lats, _ = fourier.shape
    _, pairs, length = legendre.shape
    half = length // 2
    chunks = half // LANE
    rows = n * n * SUB
    groups = len(GROUPS)
    q1, q2 = row_orders(n)
    bf16, f32 = jnp.bfloat16, jnp.float32
    vmem, dma = pltpu.VMEM, pltpu.SemaphoreType.DMA
    hbm = pl.BlockSpec(memory_space=pltpu.HBM)
    smem = pl.BlockSpec(memory_space=pltpu.SMEM)
    exchange = (chunks + 2, n, SUB, n, LANE)
    spectra, energy = pl.pallas_call(
        functools.partial(kernel, n, nz),
        out_shape=(
            jax.ShapeDtypeStruct((ch, length), f32),
            jax.ShapeDtypeStruct((1, 1), f32),
        ),
        in_specs=[hbm] * 7,
        out_specs=(hbm, smem),
        scratch_shapes=[
            vmem((ch, lats, M_WIN), bf16),
            vmem((ch * lats, M_WIN), f32),
            vmem((SUB, pairs, half), bf16),
            vmem((1, pairs), jnp.int32),
            pltpu.SMEM((pairs,), jnp.int32),
            pltpu.SMEM((lats,), f32),
            vmem((rows, rows), bf16),
            vmem((rows, rows), bf16),
            vmem((nz, SUB, ch, M_WIN), bf16),
            vmem((nz, SUB, ch, M_WIN), bf16),
            vmem(exchange, bf16),
            vmem(exchange, bf16),
            vmem(exchange, bf16),
            vmem(exchange, bf16),
            vmem((chunks, *exchange[1:]), bf16),
            vmem((chunks, rows, LANE), bf16),
            vmem((nz, ch, length), f32),
            vmem((2, ch, length), f32),
            vmem((2, ch, half), f32),
            vmem((2, ch, length), f32),
            vmem((4, ch, length), f32),
            vmem((ch, length), f32),
            vmem((nz * 2, 8, LANE), f32),
            vmem((n, 8, LANE), f32),
            vmem((n, 8, LANE), f32),
            dma((8,)),
            dma,
            dma,
            dma((groups,)),
            dma((groups,)),
            dma((groups,)),
            dma((groups,)),
            dma((groups,)),
            dma((groups,)),
            dma((4,)),
            dma((4,)),
            dma((4,)),
            dma((4,)),
            dma((3,)),
            dma((3,)),
        ],
        compiler_params=pltpu.CompilerParams(
            collective_id=0, has_side_effects=True, vmem_limit_bytes=67_043_328
        ),
        name="legendre",
    )(fourier, quad_weights, legendre, owner_pair.reshape(1, pairs), owner_pair, jnp.asarray(q1, bf16), jnp.asarray(q2, bf16))
    return spectra[None], energy[0, 0]


def solution(mesh):
    n = round(mesh.shape["lat"] ** 0.5)
    nz = mesh.shape["lev"] // 2
    finer = Mesh(mesh.devices.reshape(n, n, nz, 2), LAT + LEV)
    return jax.shard_map(
        functools.partial(shards, n, nz),
        mesh=finer,
        in_specs=(P(LEV, LAT, None), P(LAT), P(LAT, None, None), P()),
        out_specs=(P(LAT, LEV, None), P()),
        check_vma=False,
    )
```

```python
import functools

import jax
import jax.numpy as jnp
import numpy as np
from jax import lax
from jax.experimental import pallas as pl
from jax.experimental.pallas import tpu as pltpu
from jax.sharding import Mesh
from jax.sharding import PartitionSpec as P

MESH = pl.DeviceIdType.MESH
TRUNC = 1280
M_WIN = 128
SPACING = 10
LAT = ("lat_0", "lat_1")
LEV = ("lev_0", "lev_1")
LANE = 128
SUB = 5
GROUPS = ((0, 1), (1, 3), (3, 5), (5, 6), (6, 7))
TABLE_GROUPS = (0, 1, 2)
WAVE_GROUPS = (3, 4)


def row_orders(n):
    rows = n * n * SUB
    r = np.arange(rows)
    b, src, l = r // (n * SUB), r // SUB % n, r % SUB
    q1 = np.zeros((rows, rows), np.float32)
    q1[r, src * n * SUB + l * n + b] = 1
    q2 = np.zeros((rows, rows), np.float32)
    q2[r, src * n * SUB + b * SUB + l] = 1
    return q1, q2


def kernel(n, nz, f_hbm, w_hbm, leg_hbm, pair_row_hbm, pair_hbm, q1_hbm, q2_hbm, out_hbm, energy_ref,
           f_in, f_rows, tin, pair_row, pair_smem, w_smem, q1, q2, z_send, z_recv, p1s, p1r, p2s, p2r, t_sib,
           t_perm, part, a3, a4, merged, fin, out_buf, e0, e1,
           load_sem, zs_sem, zr_sem, p1s_sem, p1r_sem, p2s_sem, p2r_sem, t_ssem, t_rsem,
           a_ssem, a_rsem, f_ssem, f_rsem, e_ssem, e_rsem):
    x, y, z, c = (lax.axis_index(a) for a in LAT + LEV)
    ch = f_in.shape[0]
    part_ch = ch // 2
    half = tin.shape[2]
    chunks = half // LANE
    other = 1 - c
    pairs = n * n
    rows_of = n * n * SUB

    def core_xy(first, j):
        along_x = (c == 0) if first else (c == 1)
        return (jnp.where(along_x, j, x), jnp.where(along_x, y, j), z, c)

    me_first = jnp.where(c == 0, x, y)
    me_second = jnp.where(c == 0, y, x)

    def wrap(v, size):
        return lax.rem(v + size, size)

    loads = [
        pltpu.make_async_copy(f_hbm, f_in, load_sem.at[0]),
        pltpu.make_async_copy(pair_row_hbm, pair_row, load_sem.at[2]),
        pltpu.make_async_copy(
            leg_hbm.at[pl.ds(SUB * z, SUB), :, pl.ds(pl.multiple_of(c * half, LANE), half)], tin, load_sem.at[1]
        ),
        pltpu.make_async_copy(q1_hbm, q1, load_sem.at[3]),
        pltpu.make_async_copy(w_hbm, w_smem, load_sem.at[5]),
        pltpu.make_async_copy(pair_hbm, pair_smem, load_sem.at[6]),
        pltpu.make_async_copy(q2_hbm, q2, load_sem.at[4]),
    ]
    for load in loads:
        load.start()
    f_load, pair_row_load, table_load, q1_load, w_load, pair_load, q2_load = loads

    barrier = pltpu.get_barrier_semaphore()
    count = 0
    for r in range(1, n):
        pl.semaphore_signal(barrier, inc=1, device_id=(wrap(x + r, n), y, z, c), device_id_type=MESH)
        pl.semaphore_signal(barrier, inc=1, device_id=(x, wrap(y + r, n), z, c), device_id_type=MESH)
        count += 2
    for r in range(1, nz):
        pl.semaphore_signal(barrier, inc=1, device_id=(x, y, wrap(z + r, nz), c), device_id_type=MESH)
        pl.semaphore_signal(barrier, inc=1, device_id=(x, y, wrap(z + r, nz), other), device_id_type=MESH)
        count += 2
    pl.semaphore_signal(barrier, inc=1, device_id=(x, y, z, other), device_id_type=MESH)
    count += 1

    def remote(src, dst, ssem, rsem, device):
        return pltpu.make_async_remote_copy(
            src_ref=src, dst_ref=dst, send_sem=ssem, recv_sem=rsem, device_id=device, device_id_type=MESH
        )

    f_load.wait()
    lats = f_in.shape[1]
    f_rows[...] = f_in[...].astype(jnp.float32).reshape(ch * lats, M_WIN)
    for l in range(lats):
        rows = f_rows[pl.ds(l, ch, stride=lats), :].astype(jnp.bfloat16)
        for w in range(2):
            z_send[w, l // SUB, l % SUB] = rows[w * part_ch : (w + 1) * part_ch]
    z_recv[:, z] = z_send[:, z]

    pl.semaphore_wait(barrier, count)

    far_first = [r for k in range(n // 2, 0, -1) for r in sorted({k, n - k})]
    z_far_first = [r for k in range(nz // 2, 0, -1) for r in sorted({k, nz - k})]
    for w in range(2):
        for r in z_far_first:
            t = wrap(z + r, nz)
            remote(z_send.at[w, t], z_recv.at[w, z], zs_sem.at[w], zr_sem.at[w], (x, y, t, c)).start()

    pair_row_load.wait()
    row_i = lax.broadcasted_iota(jnp.int32, (pairs, pairs), 0)
    col_i = lax.broadcasted_iota(jnp.int32, (pairs, pairs), 1)
    owner_of_col = jnp.where(c == 0, col_i, lax.rem(col_i, n) * n + lax.div(col_i, n))
    order = jnp.where(row_i == owner_of_col, 1.0, 0.0).astype(jnp.bfloat16)
    wave_i = lax.broadcasted_iota(jnp.int32, (M_WIN, pairs), 0)
    ids = jnp.broadcast_to(pair_row[...], (M_WIN, pairs))
    low_hot = jnp.where(wave_i == ids, 1.0, 0.0).astype(jnp.bfloat16)
    high_hot = jnp.where(M_WIN - 1 - wave_i == ids, 1.0, 0.0).astype(jnp.bfloat16)

    def nt(a, b):
        return lax.dot_general(a, b, (((1,), (1,)), ((), ())), preferred_element_type=jnp.float32)

    low_sel = nt(order, low_hot).astype(jnp.bfloat16)
    high_sel = nt(order, high_hot).astype(jnp.bfloat16)

    def send_first(g):
        j0, j1 = GROUPS[g]
        p1r[j0:j1, me_first] = p1s[j0:j1, me_first]
        for r in far_first:
            t = wrap(me_first + r, n)
            remote(
                p1s.at[j0:j1, t], p1r.at[j0:j1, me_first], p1s_sem.at[g], p1r_sem.at[g], core_xy(True, t)
            ).start()

    def forward(g):
        j0, j1 = GROUPS[g]
        if n > 1:
            got = p1r.at[j0:j1, 0 : n - 1]
            remote(got, got, p1s_sem.at[g], p1r_sem.at[g], core_xy(True, me_first)).wait_recv()
        for j in range(j0, j1):
            rows = p1r[j].reshape(rows_of, LANE)
            p2s[j] = jnp.dot(q1[...], rows, preferred_element_type=jnp.float32).astype(jnp.bfloat16).reshape(p2s.shape[1:])
        p2r[j0:j1, me_second] = p2s[j0:j1, me_second]
        for r in far_first:
            t = wrap(me_second + r, n)
            remote(
                p2s.at[j0:j1, t], p2r.at[j0:j1, me_second], p2s_sem.at[g], p2r_sem.at[g], core_xy(False, t)
            ).start()

    def received_second(g):
        j0, j1 = GROUPS[g]
        if n > 1:
            got = p2r.at[j0:j1, 0 : n - 1]
            remote(got, got, p2s_sem.at[g], p2r_sem.at[g], core_xy(False, me_second)).wait_recv()

    table_load.wait()
    table_sel = low_sel[:, 0:pairs]
    for g in TABLE_GROUPS:
        j0, j1 = GROUPS[g]
        for l in range(SUB):
            rows = jnp.dot(table_sel, tin[l, :, j0 * LANE : j1 * LANE], preferred_element_type=jnp.float32)
            rows = rows.astype(jnp.bfloat16)
            for j in range(j0, j1):
                at = (j - j0) * LANE
                p1s[j, :, l] = rows[:, at : at + LANE].reshape(n, n, LANE)
        send_first(g)

    for load in (q1_load, w_load, pair_load, q2_load):
        load.wait()
    forward(0)

    def send_waves(w):
        if nz > 1:
            got = z_recv.at[w, 0 : nz - 1]
            remote(got, got, zs_sem.at[w], zr_sem.at[w], (x, y, z, c)).wait_recv()
        for l in range(SUB):
            block = z_recv[w, :, l].reshape(nz * part_ch, M_WIN)
            both = jnp.concatenate([nt(low_sel, block), nt(high_sel, block)], axis=1)
            p1s[chunks + w, :, l] = (both * w_smem[SUB * z + l]).astype(jnp.bfloat16).reshape(n, n, LANE)
        send_first(WAVE_GROUPS[w])

    send_waves(0)
    send_waves(1)
    for g in TABLE_GROUPS[1:]:
        forward(g)
    forward(WAVE_GROUPS[0])
    forward(WAVE_GROUPS[1])

    swaps = []
    for g in TABLE_GROUPS:
        received_second(g)
        j0, j1 = GROUPS[g]
        swap = remote(p2r.at[j0:j1], t_sib.at[j0:j1], t_ssem.at[g], t_rsem.at[g], (x, y, z, other))
        swap.start()
        swaps.append(swap)
    for g in TABLE_GROUPS:
        swaps[g].wait_recv()
        for j in range(*GROUPS[g]):
            rows = t_sib[j].reshape(rows_of, LANE)
            t_perm[j] = jnp.dot(q2[...], rows, preferred_element_type=jnp.float32).astype(jnp.bfloat16)

    limit = TRUNC - SPACING * pair_smem[x * n + y] - SPACING // 2

    def product(w):
        received_second(WAVE_GROUPS[w])
        waves = p2r[chunks + w].reshape(rows_of, LANE)
        low = LANE // 2
        for j in range(0, 2 * chunks, 2):
            blocks = [p2r[i].reshape(rows_of, LANE) if i < chunks else t_perm[i - chunks] for i in (j, j + 1)]
            table = jnp.concatenate(blocks, axis=1)
            both = lax.dot_general(waves, table, (((0,), (0,)), ((), ())), preferred_element_type=jnp.float32)
            for i in range(2):
                first = c * half + (j + i) * LANE if j + i < chunks else other * half + (j + i - chunks) * LANE
                column = first + lax.broadcasted_iota(jnp.int32, (low, LANE), 1)
                at = i * LANE
                sums = jnp.where(column < limit, both[:low, at : at + LANE], both[low:, at : at + LANE])
                part[w, :, :, (j + i) * LANE : (j + i + 1) * LANE] = sums.reshape(nz, part_ch, LANE)

    def up(k):
        return wrap(z + k + nz, nz)

    ways = ((0, 1), (1, -1)) if nz > 1 else ()

    def send_part(w):
        sends = []
        for i, sign in ways:
            sends.append(remote(
                part.at[w, up(3 * sign)], a3.at[w, i], a_ssem.at[w, i], a_rsem.at[w, i], (x, y, up(sign), c)
            ))
            sends.append(remote(
                part.at[w, up(4), :, i * half : (i + 1) * half], a4.at[w, i], a_ssem.at[w, 2 + i],
                a_rsem.at[w, 2 + i], (x, y, up(2 * sign), c),
            ))
        for i, sign in ways:
            sends.append(remote(
                part.at[w, up(sign)], fin.at[w, i], f_ssem.at[w, i], f_rsem.at[w, i], (x, y, up(sign), c)
            ))
        for send in sends:
            send.start()
        return sends

    def merge(w, sends):
        for i, sign in ways:
            sends[2 * i].wait_recv()
            merged[w, i] = part[w, up(2 * sign)] + a3[w, i]
            sends[2 * i + 1].wait_recv()
            at = slice(i * half, (i + 1) * half)
            merged[w, i, :, at] = merged[w, i, :, at] + a4[w, i]
            send = remote(
                merged.at[w, i], fin.at[w, 2 + i], f_ssem.at[w, 2 + i], f_rsem.at[w, 2 + i], (x, y, up(2 * sign), c)
            )
            send.start()
            sends.append(send)

    def final(w, sends):
        total = part[w, z]
        for send in sends[4:]:
            send.wait_recv()
        for i in range(4 if nz > 1 else 0):
            total = total + fin[w, i]
        return total

    product(0)
    sends0 = send_part(0)
    product(1)
    sends1 = send_part(1)
    merge(0, sends0)
    merge(1, sends1)
    total0 = final(0, sends0)
    total1 = final(1, sends1)
    total = jnp.concatenate([total0, total1], axis=0)
    sends = sends0 + sends1

    levels = nz * 2 * ch // 2
    channel = (z * 2 + c) * ch + lax.broadcasted_iota(jnp.int32, (ch, LANE), 0)
    factor = 1.0 + 2.0 * lax.shift_right_logical(channel, 1).astype(jnp.float32) / (levels - 1)
    columns = [total[:, j * LANE : (j + 1) * LANE] for j in range(2 * chunks)]
    squares = columns[0] * columns[0]
    for column in columns[1:]:
        squares = squares + column * column
    squares = factor * squares
    tile = squares[0:8]
    for i in range(1, ch // 8):
        tile = tile + squares[i * 8 : i * 8 + 8]

    def share(ref, at, tile, sem, devices):
        ref[at] = tile
        for device in devices:
            remote(ref.at[at], ref.at[at], e_ssem.at[sem], e_rsem.at[sem], device).start()

    def added(ref, size, sem):
        if size > 1:
            got = ref.at[0 : size - 1]
            remote(got, got, e_ssem.at[sem], e_rsem.at[sem], (x, y, z, c)).wait_recv()
        tile = ref[0]
        for i in range(1, size):
            tile = tile + ref[i]
        return tile

    peers = [(x, y, wrap(z + r, nz), k) for r in z_far_first for k in (c, other)] + [(x, y, z, other)]
    share(e0, z * 2 + c, tile, 0, peers)
    out_buf[:, pl.ds(pl.multiple_of(c * half, LANE), half)] = total[:, :half]
    out_buf[:, pl.ds(pl.multiple_of(other * half, LANE), half)] = total[:, half:]
    out_copy = pltpu.make_async_copy(out_buf, out_hbm, load_sem.at[7])
    out_copy.start()
    tile = added(e0, nz * 2, 0)
    tile = jnp.sum(tile, axis=0, keepdims=True)
    ring = [min(r, n - r) for r in range(n)]
    steps = sorted(((i, j) for i in range(n) for j in range(n) if i or j), key=lambda s: -ring[s[0]] - ring[s[1]])
    share(e1, x * n + y, tile, 1, [(wrap(x + i, n), wrap(y + j, n), z, c) for i, j in steps])
    tile = added(e1, pairs, 1)
    energy_ref[0, 0] = jnp.sum(tile) / (pairs * 2 * levels * 2 * half)

    out_copy.wait()
    if nz > 1:
        for w in range(2):
            gone = z_send.at[w, 0 : nz - 1]
            remote(gone, gone, zs_sem.at[w], zr_sem.at[w], (x, y, z, c)).wait_send()
    if n > 1:
        for g, (j0, j1) in enumerate(GROUPS):
            gone = p1s.at[j0:j1, 0 : n - 1]
            remote(gone, gone, p1s_sem.at[g], p1r_sem.at[g], (x, y, z, c)).wait_send()
            gone = p2s.at[j0:j1, 0 : n - 1]
            remote(gone, gone, p2s_sem.at[g], p2r_sem.at[g], (x, y, z, c)).wait_send()
    for send in swaps + sends:
        send.wait_send()
    for sem, ref, size in ((0, e0, nz * 2), (1, e1, pairs)):
        if size > 1:
            gone = ref.at[0 : size - 1]
            remote(gone, gone, e_ssem.at[sem], e_rsem.at[sem], (x, y, z, c)).wait_send()


def shards(n, nz, fourier, quad_weights, legendre, owner_pair):
    ch, lats, _ = fourier.shape
    _, pairs, length = legendre.shape
    half = length // 2
    chunks = half // LANE
    rows = n * n * SUB
    groups = len(GROUPS)
    q1, q2 = row_orders(n)
    bf16, f32 = jnp.bfloat16, jnp.float32
    vmem, dma = pltpu.VMEM, pltpu.SemaphoreType.DMA
    hbm = pl.BlockSpec(memory_space=pltpu.HBM)
    smem = pl.BlockSpec(memory_space=pltpu.SMEM)
    exchange = (chunks + 2, n, SUB, n, LANE)
    spectra, energy = pl.pallas_call(
        functools.partial(kernel, n, nz),
        out_shape=(
            jax.ShapeDtypeStruct((ch, length), f32),
            jax.ShapeDtypeStruct((1, 1), f32),
        ),
        in_specs=[hbm] * 7,
        out_specs=(hbm, smem),
        scratch_shapes=[
            vmem((ch, lats, M_WIN), bf16),
            vmem((ch * lats, M_WIN), f32),
            vmem((SUB, pairs, half), bf16),
            vmem((1, pairs), jnp.int32),
            pltpu.SMEM((pairs,), jnp.int32),
            pltpu.SMEM((lats,), f32),
            vmem((rows, rows), bf16),
            vmem((rows, rows), bf16),
            vmem((2, nz, SUB, ch // 2, M_WIN), bf16),
            vmem((2, nz, SUB, ch // 2, M_WIN), bf16),
            vmem(exchange, bf16),
            vmem(exchange, bf16),
            vmem(exchange, bf16),
            vmem(exchange, bf16),
            vmem((chunks, *exchange[1:]), bf16),
            vmem((chunks, rows, LANE), bf16),
            vmem((2, nz, ch // 2, length), f32),
            vmem((2, 2, ch // 2, length), f32),
            vmem((2, 2, ch // 2, half), f32),
            vmem((2, 2, ch // 2, length), f32),
            vmem((2, 4, ch // 2, length), f32),
            vmem((ch, length), f32),
            vmem((nz * 2, 8, LANE), f32),
            vmem((n * n, 1, LANE), f32),
            dma((8,)),
            dma((2,)),
            dma((2,)),
            dma((groups,)),
            dma((groups,)),
            dma((groups,)),
            dma((groups,)),
            dma((groups,)),
            dma((groups,)),
            dma((2, 4)),
            dma((2, 4)),
            dma((2, 4)),
            dma((2, 4)),
            dma((2,)),
            dma((2,)),
        ],
        compiler_params=pltpu.CompilerParams(
            collective_id=0, has_side_effects=True, vmem_limit_bytes=67_043_328
        ),
        name="legendre",
    )(fourier, quad_weights, legendre, owner_pair.reshape(1, pairs), owner_pair, jnp.asarray(q1, bf16), jnp.asarray(q2, bf16))
    return spectra[None], energy[0, 0]


def solution(mesh):
    n = round(mesh.shape["lat"] ** 0.5)
    nz = mesh.shape["lev"] // 2
    finer = Mesh(mesh.devices.reshape(n, n, nz, 2), LAT + LEV)
    return jax.shard_map(
        functools.partial(shards, n, nz),
        mesh=finer,
        in_specs=(P(LEV, LAT, None), P(LAT), P(LAT, None, None), P()),
        out_specs=(P(LAT, LEV, None), P()),
        check_vma=False,
    )
```

```python
import functools

import jax
import jax.numpy as jnp
from jax import lax
from jax.experimental import pallas as pl
from jax.experimental.pallas import tpu as pltpu
from jax.sharding import Mesh
from jax.sharding import PartitionSpec as P

MESH = pl.DeviceIdType.MESH
TRUNC = 1280
M_WIN = 128
SPACING = 10
LAT = ("lat_0", "lat_1")
LEV = ("lev_0", "lev_1")
LANE = 128
PIECES = ((0, 3), (3, 5))


def nt(a, b):
    return lax.dot_general(a, b, (((1,), (1,)), ((), ())), preferred_element_type=jnp.float32)


def tn(a, b):
    return lax.dot_general(a, b, (((0,), (0,)), ((), ())), preferred_element_type=jnp.float32)


def one_hot(condition):
    return jnp.where(condition, 1.0, 0.0).astype(jnp.bfloat16)


def iota(shape, dim):
    return lax.broadcasted_iota(jnp.int32, shape, dim)


def lanes_for_rows(tiles, rows, width):
    row, lane = iota(tiles.shape, 1), iota(tiles.shape, 2)
    group = lax.div(lane, width)
    step = 1
    while step < rows:
        row_bit, group_bit = lax.rem(lax.div(row, step), 2), lax.rem(lax.div(group, step), 2)
        down = pltpu.roll(pltpu.roll(tiles, step, 1), LANE - step * width, 2)
        up = pltpu.roll(pltpu.roll(tiles, rows - step, 1), step * width, 2)
        moved = jnp.where(row_bit > group_bit, down, up)
        tiles = jnp.where(row_bit == group_bit, tiles, moved)
        step *= 2
    return tiles


def kernel(n, f_hbm, w_hbm, leg_hbm, pair_row_hbm, pair_hbm, out_hbm, energy_ref,
           f_in, f_rows, g, tin, pair_row, pair_smem, w_smem, z_send, z_recv, w_send, w_recv, t_send, t_recv,
           part, a3, a4, merged, fin, total_ref, e0, e1,
           load_sem, zs_sem, zr_sem, ws_sem, wr_sem, ts_sem, tr_sem,
           a_ssem, a_rsem, f_ssem, f_rsem, o_ssem, o_rsem, e_ssem, e_rsem):
    x, y, z, c = (lax.axis_index(a) for a in LAT + LEV)
    ch, lats, _ = f_in.shape
    half = tin.shape[2]
    chunks = half // LANE
    other = 1 - c
    pairs = n * n
    sources = 2 * n
    width = ch
    rows = LANE // width
    blocks = lats // rows
    sides = sources // rows
    me = z * 2 + c

    def first_axis(j):
        return (jnp.where(c == 0, j, x), jnp.where(c == 0, y, j), z, c)

    def second_axis(j):
        return (jnp.where(c == 0, x, j), jnp.where(c == 0, j, y), z, c)

    me_first = jnp.where(c == 0, x, y)
    me_second = jnp.where(c == 0, y, x)

    def wrap(v):
        return lax.rem(v + n, n)

    loads = [
        pltpu.make_async_copy(f_hbm, f_in, load_sem.at[0]),
        pltpu.make_async_copy(pair_row_hbm, pair_row, load_sem.at[1]),
        pltpu.make_async_copy(w_hbm, w_smem, load_sem.at[2]),
        pltpu.make_async_copy(leg_hbm.at[:, :, pl.ds(pl.multiple_of(c * half, LANE), half)], tin, load_sem.at[3]),
        pltpu.make_async_copy(pair_hbm, pair_smem, load_sem.at[4]),
    ]
    for load in loads:
        load.start()
    f_load, pair_row_load, w_load, table_load, pair_load = loads

    barrier = pltpu.get_barrier_semaphore()
    count = 0
    far_first = [r for k in range(n // 2, 0, -1) for r in sorted({k, n - k})]
    for r in far_first:
        for device in (
            (wrap(x + r), y, z, c), (x, wrap(y + r), z, c), (x, y, wrap(z + r), c), (x, y, wrap(z + r), other)
        ):
            pl.semaphore_signal(barrier, inc=1, device_id=device, device_id_type=MESH)
            count += 1
    pl.semaphore_signal(barrier, inc=1, device_id=(x, y, z, other), device_id_type=MESH)
    count += 1

    def remote(src, dst, ssem, rsem, device):
        return pltpu.make_async_remote_copy(
            src_ref=src, dst_ref=dst, send_sem=ssem, recv_sem=rsem, device_id=device, device_id_type=MESH
        )

    f_load.wait()
    f_rows[...] = f_in[...].astype(jnp.float32).reshape(ch * lats, M_WIN)
    for l in range(lats):
        g[l // rows, l % rows * ch : (l % rows + 1) * ch] = f_rows[pl.ds(l, ch, stride=lats), :].astype(jnp.bfloat16)

    pair_row_load.wait()
    row_i, col_i = iota((pairs, pairs), 0), iota((pairs, pairs), 1)
    swapped = one_hot(row_i == lax.rem(col_i, n) * n + lax.div(col_i, n))
    wave_i = iota((M_WIN, pairs), 0)
    ids = jnp.broadcast_to(pair_row[...], (M_WIN, pairs))
    low_hot = one_hot(wave_i == ids)
    high_hot = one_hot(M_WIN - 1 - wave_i == ids)
    plain = one_hot(row_i == col_i)
    sel = jnp.concatenate([nt(swapped, low_hot), nt(plain, low_hot), nt(plain, high_hot)], axis=0).astype(jnp.bfloat16)
    for b in range(blocks):
        got = nt(sel, g[b]).astype(jnp.bfloat16)
        z_send[:, :, b] = got.reshape(3, n, n, LANE)
    z_recv[0, me] = z_send[c, z]
    z_recv[1, me] = z_send[2, z]

    pl.semaphore_wait(barrier, count)

    def z_copy(kind, u, t, core):
        remote(z_send.at[kind, t], z_recv.at[u, me], zs_sem.at[u], zr_sem.at[u], (x, y, t, core)).start()

    for core in (1, 0):
        for r in far_first:
            z_copy(core, 0, wrap(z + r), core)
    z_copy(other, 0, z, other)
    for r in far_first:
        z_copy(2, 1, wrap(z + r), 1)

    @pl.when(c == 0)
    def _():
        z_copy(2, 1, z, 1)

    table_rows = n * rows
    device_i = lax.div(iota((table_rows, pairs), 0), rows)
    owner_i = jnp.where(c == 0, device_i * n + z, z * n + device_i)
    owner_of_row = one_hot(iota((table_rows, pairs), 1) == owner_i)
    depth = rows * pairs
    pair_of = lax.rem(iota((depth, pairs), 0), pairs)
    table_hot = one_hot(pair_of == jnp.broadcast_to(pair_row[...], (depth, pairs)))
    same_lat = lax.rem(iota((table_rows, depth), 0), rows) == lax.div(iota((table_rows, depth), 1), pairs)
    pick = jnp.where(same_lat, nt(owner_of_row, table_hot), 0.0).astype(jnp.bfloat16)
    table_load.wait()
    for b in range(blocks):
        block = tin[b * rows : (b + 1) * rows].reshape(depth, half)
        got = jnp.dot(pick, block, preferred_element_type=jnp.float32).astype(jnp.bfloat16)
        t_send[:, b] = got.reshape(n, rows, half)
    t_recv[me_first] = t_send[me_first]
    for r in far_first:
        t = wrap(me_first + r)
        remote(t_send.at[t], t_recv.at[me_first], ts_sem, tr_sem, first_axis(t)).start()

    w_load.wait()
    pair_load.wait()
    weight_row = iota((rows, LANE), 0)
    weights = []
    for b in range(blocks):
        weight = jnp.zeros((rows, LANE), jnp.float32)
        for l in range(rows):
            weight = jnp.where(weight_row == l, w_smem[b * rows + l], weight)
        weights.append(weight)
    side = sources * n
    order_i = iota((side, side), 0)
    by_device = one_hot(iota((side, side), 1) == lax.rem(order_i, sources) * n + lax.div(order_i, sources))

    def send_waves(u):
        got = z_recv.at[u, 0 : sources - 1]
        remote(got, got, zs_sem.at[u], zr_sem.at[u], (x, y, z, c)).wait_recv()
        for b in range(blocks):
            tiles = jnp.dot(by_device, z_recv[u, :, b].reshape(side, LANE), preferred_element_type=jnp.float32)
            tiles = lanes_for_rows(tiles.reshape(n * sides, rows, LANE), rows, width)
            w_send[u, :, :, b] = (tiles * weights[b][None]).astype(jnp.bfloat16).reshape(n, sides, rows, LANE)
        w_recv[u, me_first] = w_send[u, me_first]
        for r in far_first:
            t = wrap(me_first + r)
            remote(w_send.at[u, t], w_recv.at[u, me_first], ws_sem.at[u], wr_sem.at[u], first_axis(t)).start()

    def wait_waves(u):
        got = w_recv.at[u, 0 : n - 1]
        remote(got, got, ws_sem.at[u], wr_sem.at[u], (x, y, z, c)).wait_recv()

    send_waves(0)

    @pl.when(c == 1)
    def _():
        send_waves(1)

    got = t_recv.at[0 : n - 1]
    remote(got, got, ts_sem, tr_sem, (x, y, z, c)).wait_recv()
    wait_waves(0)

    @pl.when(c == 1)
    def _():
        wait_waves(1)

    depth_all = n * lats
    pair_id = pair_smem[jnp.where(c == 0, x * n + z, z * n + y)]
    limit = TRUNC - SPACING * pair_id - SPACING // 2

    def waves_of(u):
        return jnp.concatenate([w_recv[u, :, s].reshape(depth_all, LANE) for s in range(sides)], axis=1)

    def table_of(j0, j1):
        return t_recv[:, :, :, j0 * LANE : j1 * LANE].reshape(depth_all, (j1 - j0) * LANE)

    low_waves = waves_of(0)

    def product(j0, j1):
        spans = [(j, min(j + 2, j1)) for j in range(j0, j1, 2)]

        @pl.when(c == 0)
        def _():
            for k0, k1 in spans:
                sums = tn(low_waves, table_of(k0, k1))
                part[:, :, k0 * LANE : k1 * LANE] = sums.reshape(n, 2 * ch, (k1 - k0) * LANE)

        @pl.when(c == 1)
        def _():
            high_waves = waves_of(1)
            for k0, k1 in spans:
                table = table_of(k0, k1)
                column = half + k0 * LANE + iota((sources * ch, (k1 - k0) * LANE), 1)
                sums = jnp.where(column < limit, tn(low_waves, table), tn(high_waves, table))
                part[:, :, k0 * LANE : k1 * LANE] = sums.reshape(n, 2 * ch, (k1 - k0) * LANE)

    def up(k):
        return wrap(me_second + k)

    far = n == 8
    ways = ((1, -1), (0, 1)) if far else ((0, 1),)
    stage, near, late = {}, {}, {}

    def span_of(p):
        return slice(PIECES[p][0] * LANE, PIECES[p][1] * LANE)

    def send_far(p):
        at = span_of(p)
        for i, sign in ways if far else ():
            stage[p, i] = (
                remote(
                    part.at[up(3 * sign), :, at], a3.at[i, :, at], a_ssem.at[p, i], a_rsem.at[p, i],
                    second_axis(up(sign)),
                ),
                remote(
                    part.at[up(4), i * ch : (i + 1) * ch, at], a4.at[i, :, at], a_ssem.at[p, 2 + i],
                    a_rsem.at[p, 2 + i], second_axis(up(2 * sign)),
                ),
            )
            for send in stage[p, i]:
                send.start()

    def send_near(p):
        at = span_of(p)
        for i, sign in ways:
            near[p, i] = remote(
                part.at[up(sign), :, at], fin.at[i, :, at], f_ssem.at[p, i], f_rsem.at[p, i], second_axis(up(sign))
            )
            near[p, i].start()

    def merge(p):
        at = span_of(p)
        for i, sign in ways if far else ():
            stage[p, i][0].wait_recv()
            merged[i, :, at] = part[up(2 * sign), :, at] + a3[i, :, at]
            stage[p, i][1].wait_recv()
            mine = slice(i * ch, (i + 1) * ch)
            merged[i, mine, at] = merged[i, mine, at] + a4[i, :, at]
            late[p, i] = remote(
                merged.at[i, :, at], fin.at[2 + i, :, at], f_ssem.at[p, 2 + i], f_rsem.at[p, 2 + i],
                second_axis(up(2 * sign)),
            )
            late[p, i].start()

    def final(p):
        at = span_of(p)
        total = part[me_second, :, at]
        for i, _ in ways:
            near[p, i].wait_recv()
            total = total + fin[i, :, at]
        for i, _ in ways if far else ():
            late[p, i].wait_recv()
            total = total + fin[2 + i, :, at]
        return total

    product(*PIECES[0])
    send_far(0)
    product(*PIECES[1])
    send_far(1)
    send_near(0)
    merge(0)
    send_near(1)
    merge(1)
    total = jnp.concatenate([final(0), final(1)], axis=1)

    levels = sources * ch // 2
    channel = me_second * 2 * ch + iota((2 * ch, LANE), 0)
    factor = 1.0 + 2.0 * lax.shift_right_logical(channel, 1).astype(jnp.float32) / (levels - 1)
    squares = None
    for j in range(chunks):
        column = total[:, j * LANE : (j + 1) * LANE]
        squares = column * column if squares is None else squares + column * column
    squares = factor * squares
    tile = squares[0:8]
    for i in range(1, 2 * ch // 8):
        tile = tile + squares[i * 8 : i * 8 + 8]

    def share(ref, at, tile, sem, devices):
        ref[at] = tile
        for device in devices:
            remote(ref.at[at], ref.at[at], e_ssem.at[sem], e_rsem.at[sem], device).start()

    def added(ref, size, sem):
        got = ref.at[0 : size - 1]
        remote(got, got, e_ssem.at[sem], e_rsem.at[sem], (x, y, z, c)).wait_recv()
        tile = ref[0]
        for i in range(1, size):
            tile = tile + ref[i]
        return tile

    peers = [(x, y, wrap(z + r), k) for r in far_first for k in (c, other)] + [(x, y, z, other)]
    share(e0, me, tile, 0, peers)
    total_ref[...] = total

    tile = added(e0, sources, 0)
    tile = jnp.sum(tile, axis=0, keepdims=True)
    ring = [min(r, n - r) for r in range(n)]
    steps = sorted(((i, j) for i in range(n) for j in range(n) if i or j), key=lambda s: -ring[s[0]] - ring[s[1]])
    share(e1, x * n + y, tile, 1, [(wrap(x + i), wrap(y + j), z, c) for i, j in steps])

    at_home = jnp.where(c == 0, y, x) == z

    def rows_of(core):
        return total_ref.at[pl.ds(pl.multiple_of(core * ch, 8), ch)]

    home = out_hbm.at[:, pl.ds(pl.multiple_of(c * half, LANE), half)]
    at_home_copy = pltpu.make_async_copy(rows_of(c), home, load_sem.at[5])

    def to_owner(core):
        device = (jnp.where(c == 0, x, z), jnp.where(c == 0, z, y), me_second, core)
        return remote(rows_of(core), home, o_ssem.at[core], o_rsem.at[c], device)

    to_owner(other).start()

    @pl.when(at_home)
    def _():
        at_home_copy.start()

    @pl.when(jnp.logical_not(at_home))
    def _():
        to_owner(c).start()

    tile = added(e1, pairs, 1)
    energy_ref[0, 0] = jnp.sum(tile) / (pairs * 2 * levels * 2 * half)

    def from_core(core):
        got = out_hbm.at[:, pl.ds(pl.multiple_of(core * half, LANE), half)]
        return remote(got, got, o_ssem.at[core], o_rsem.at[core], (x, y, z, c))

    from_core(other).wait_recv()

    @pl.when(at_home)
    def _():
        at_home_copy.wait()

    @pl.when(jnp.logical_not(at_home))
    def _():
        from_core(c).wait_recv()

    first = z_recv.at[0, 0 : sources - 1]
    remote(first, first, zs_sem.at[0], zr_sem.at[0], (x, y, z, c)).wait_send()

    @pl.when(c == 0)
    def _():
        second = z_recv.at[1, 0:n]
        remote(second, second, zs_sem.at[1], zr_sem.at[1], (x, y, z, c)).wait_send()

    @pl.when(c == 1)
    def _():
        second = z_recv.at[1, 0 : n - 1]
        remote(second, second, zs_sem.at[1], zr_sem.at[1], (x, y, z, c)).wait_send()
        gone = w_send.at[1, 0 : n - 1]
        remote(gone, gone, ws_sem.at[1], wr_sem.at[1], (x, y, z, c)).wait_send()

    gone = w_send.at[0, 0 : n - 1]
    remote(gone, gone, ws_sem.at[0], wr_sem.at[0], (x, y, z, c)).wait_send()
    gone = t_send.at[0 : n - 1]
    remote(gone, gone, ts_sem, tr_sem, (x, y, z, c)).wait_send()
    for key in near:
        near[key].wait_send()
    for key in late:
        stage[key][0].wait_send()
        stage[key][1].wait_send()
        late[key].wait_send()
    to_owner(other).wait_send()

    @pl.when(jnp.logical_not(at_home))
    def _():
        to_owner(c).wait_send()

    for sem, ref, size in ((0, e0, sources), (1, e1, pairs)):
        gone = ref.at[0 : size - 1]
        remote(gone, gone, e_ssem.at[sem], e_rsem.at[sem], (x, y, z, c)).wait_send()


def shards(n, fourier, quad_weights, legendre, owner_pair):
    ch, lats, _ = fourier.shape
    _, pairs, length = legendre.shape
    half = length // 2
    rows = LANE // ch
    blocks = lats // rows
    sides = 2 * n // rows
    bf16, f32 = jnp.bfloat16, jnp.float32
    vmem, dma = pltpu.VMEM, pltpu.SemaphoreType.DMA
    hbm = pl.BlockSpec(memory_space=pltpu.HBM)
    smem = pl.BlockSpec(memory_space=pltpu.SMEM)
    spectra, energy = pl.pallas_call(
        functools.partial(kernel, n),
        out_shape=(
            jax.ShapeDtypeStruct((ch, length), f32),
            jax.ShapeDtypeStruct((1, 1), f32),
        ),
        in_specs=[hbm] * 5,
        out_specs=(hbm, smem),
        scratch_shapes=[
            vmem((ch, lats, M_WIN), bf16),
            vmem((ch * lats, M_WIN), f32),
            vmem((blocks, LANE, M_WIN), bf16),
            vmem((lats, pairs, half), bf16),
            vmem((1, pairs), jnp.int32),
            pltpu.SMEM((pairs,), jnp.int32),
            pltpu.SMEM((lats,), f32),
            vmem((3, n, blocks, n, LANE), bf16),
            vmem((2, 2 * n, blocks, n, LANE), bf16),
            vmem((2, n, sides, blocks, rows, LANE), bf16),
            vmem((2, n, sides, blocks, rows, LANE), bf16),
            vmem((n, blocks, rows, half), bf16),
            vmem((n, blocks, rows, half), bf16),
            vmem((n, 2 * ch, half), f32),
            vmem((2, 2 * ch, half), f32),
            vmem((2, ch, half), f32),
            vmem((2, 2 * ch, half), f32),
            vmem((4, 2 * ch, half), f32),
            vmem((2 * ch, half), f32),
            vmem((2 * n, 8, LANE), f32),
            vmem((n * n, 1, LANE), f32),
            dma((6,)),
            dma((2,)),
            dma((2,)),
            dma((2,)),
            dma((2,)),
            dma,
            dma,
            dma((2, 4)),
            dma((2, 4)),
            dma((2, 4)),
            dma((2, 4)),
            dma((2,)),
            dma((2,)),
            dma((2,)),
            dma((2,)),
        ],
        compiler_params=pltpu.CompilerParams(collective_id=0, has_side_effects=True, vmem_limit_bytes=67_043_328),
        name="legendre",
    )(fourier, quad_weights, legendre, owner_pair.reshape(1, pairs), owner_pair)
    return spectra[None], energy[0, 0]


def solution(mesh):
    n = mesh.shape["lev"] // 2
    finer = Mesh(mesh.devices.reshape(n, n, n, 2), LAT + LEV)
    return jax.shard_map(
        functools.partial(shards, n),
        mesh=finer,
        in_specs=(P(LEV, LAT, None), P(LAT), P(LAT, None, None), P()),
        out_specs=(P(LAT, LEV, None), P()),
        check_vma=False,
    )
```

```python
import functools

import jax
import jax.numpy as jnp
from jax import lax
from jax.experimental import pallas as pl
from jax.experimental.pallas import tpu as pltpu
from jax.sharding import Mesh
from jax.sharding import PartitionSpec as P

MESH = pl.DeviceIdType.MESH
TRUNC = 1280
M_WIN = 128
SPACING = 10
LAT = ("lat_0", "lat_1")
LEV = ("lev_0", "lev_1")
LANE = 128
PIECES = ((0, 3), (3, 5))


def nt(a, b):
    return lax.dot_general(a, b, (((1,), (1,)), ((), ())), preferred_element_type=jnp.float32)


def tn(a, b):
    return lax.dot_general(a, b, (((0,), (0,)), ((), ())), preferred_element_type=jnp.float32)


def one_hot(condition):
    return jnp.where(condition, 1.0, 0.0).astype(jnp.bfloat16)


def iota(shape, dim):
    return lax.broadcasted_iota(jnp.int32, shape, dim)


def lanes_for_rows(tiles, rows, width):
    row, lane = iota(tiles.shape, 1), iota(tiles.shape, 2)
    group = lax.div(lane, width)
    step = 1
    while step < rows:
        row_bit, group_bit = lax.rem(lax.div(row, step), 2), lax.rem(lax.div(group, step), 2)
        moved = pltpu.roll(pltpu.roll(tiles, rows - step, 1), step * width, 2)
        if 2 * step < rows:
            down = pltpu.roll(pltpu.roll(tiles, step, 1), LANE - step * width, 2)
            moved = jnp.where(row_bit > group_bit, down, moved)
        tiles = jnp.where(row_bit == group_bit, tiles, moved)
        step *= 2
    return tiles


def kernel(n, f_hbm, w_hbm, leg_hbm, pair_row_hbm, pair_hbm, out_hbm, e1_hbm,
           f_in, f_rows, g, tin, pair_row, pair_smem, w_smem, z_send, z_recv, w_send, w_recv, t_send, t_recv,
           part, a3, a4, merged, fin, total_ref, e0, e_row,
           load_sem, zs_sem, zr_sem, ws_sem, wr_sem, ts_sem, tr_sem,
           a_ssem, a_rsem, f_ssem, f_rsem, o_ssem, o_rsem, e_ssem, e_rsem):
    x, y, z, c = (lax.axis_index(a) for a in LAT + LEV)
    ch, lats, _ = f_in.shape
    half = tin.shape[2]
    chunks = half // LANE
    other = 1 - c
    pairs = n * n
    sources = 2 * n
    width = ch
    rows = LANE // width
    blocks = lats // rows
    sides = sources // rows
    me = z * 2 + c

    def first_axis(j):
        return (jnp.where(c == 0, j, x), jnp.where(c == 0, y, j), z, c)

    def second_axis(j):
        return (jnp.where(c == 0, x, j), jnp.where(c == 0, j, y), z, c)

    me_first = jnp.where(c == 0, x, y)
    me_second = jnp.where(c == 0, y, x)

    def wrap(v):
        return lax.rem(v + n, n)

    loads = [
        pltpu.make_async_copy(f_hbm, f_in, load_sem.at[0]),
        pltpu.make_async_copy(pair_row_hbm, pair_row, load_sem.at[1]),
        pltpu.make_async_copy(w_hbm, w_smem, load_sem.at[2]),
        pltpu.make_async_copy(leg_hbm.at[:, :, pl.ds(pl.multiple_of(c * half, LANE), half)], tin, load_sem.at[3]),
        pltpu.make_async_copy(pair_hbm, pair_smem, load_sem.at[4]),
    ]
    for load in loads:
        load.start()
    f_load, pair_row_load, w_load, table_load, pair_load = loads

    barrier = pltpu.get_barrier_semaphore()
    count = 0
    far_first = [r for k in range(n // 2, 0, -1) for r in sorted({k, n - k})]
    for r in far_first:
        for device in (
            (wrap(x + r), y, z, c), (x, wrap(y + r), z, c), (x, y, wrap(z + r), c), (x, y, wrap(z + r), other)
        ):
            pl.semaphore_signal(barrier, inc=1, device_id=device, device_id_type=MESH)
            count += 1
    pl.semaphore_signal(barrier, inc=1, device_id=(x, y, z, other), device_id_type=MESH)
    count += 1

    def remote(src, dst, ssem, rsem, device):
        return pltpu.make_async_remote_copy(
            src_ref=src, dst_ref=dst, send_sem=ssem, recv_sem=rsem, device_id=device, device_id_type=MESH
        )

    f_load.wait()
    f_rows[...] = f_in[...].astype(jnp.float32).reshape(ch * lats, M_WIN)
    for l in range(lats):
        g[l // rows, l % rows * ch : (l % rows + 1) * ch] = f_rows[pl.ds(l, ch, stride=lats), :].astype(jnp.bfloat16)

    pair_row_load.wait()
    row_i, col_i = iota((pairs, pairs), 0), iota((pairs, pairs), 1)
    swapped = one_hot(row_i == lax.rem(col_i, n) * n + lax.div(col_i, n))
    wave_i = iota((M_WIN, pairs), 0)
    ids = jnp.broadcast_to(pair_row[...], (M_WIN, pairs))
    low_hot = one_hot(wave_i == ids)
    high_hot = one_hot(M_WIN - 1 - wave_i == ids)
    plain = one_hot(row_i == col_i)
    sel = jnp.concatenate([nt(swapped, low_hot), nt(plain, low_hot), nt(plain, high_hot)], axis=0).astype(jnp.bfloat16)
    for b in range(blocks):
        got = nt(sel, g[b]).astype(jnp.bfloat16)
        z_send[:, :, b] = got.reshape(3, n, n, LANE)
    z_recv[0, me] = z_send[c, z]
    z_recv[1, me] = z_send[2, z]

    pl.semaphore_wait(barrier, count)

    def z_copy(kind, u, t, core):
        remote(z_send.at[kind, t], z_recv.at[u, me], zs_sem.at[u], zr_sem.at[u], (x, y, t, core)).start()

    for core in (0, 1):
        for r in far_first:
            z_copy(core, 0, wrap(z + r), core)
    z_copy(other, 0, z, other)
    for r in far_first:
        z_copy(2, 1, wrap(z + r), 1)

    @pl.when(c == 0)
    def _():
        z_copy(2, 1, z, 1)

    table_rows = n * rows
    device_i = lax.div(iota((table_rows, pairs), 0), rows)
    owner_i = jnp.where(c == 0, device_i * n + z, z * n + device_i)
    owner_of_row = one_hot(iota((table_rows, pairs), 1) == owner_i)
    depth = rows * pairs
    pair_of = lax.rem(iota((depth, pairs), 0), pairs)
    table_hot = one_hot(pair_of == jnp.broadcast_to(pair_row[...], (depth, pairs)))
    same_lat = lax.rem(iota((table_rows, depth), 0), rows) == lax.div(iota((table_rows, depth), 1), pairs)
    pick = jnp.where(same_lat, nt(owner_of_row, table_hot), 0.0).astype(jnp.bfloat16)
    table_load.wait()
    for b in range(blocks):
        block = tin[b * rows : (b + 1) * rows].reshape(depth, half)
        got = jnp.dot(pick, block, preferred_element_type=jnp.float32).astype(jnp.bfloat16)
        t_send[:, b] = got.reshape(n, rows, half)
    t_recv[me_first] = t_send[me_first]
    for r in far_first:
        t = wrap(me_first + r)
        remote(t_send.at[t], t_recv.at[me_first], ts_sem, tr_sem, first_axis(t)).start()

    w_load.wait()
    pair_load.wait()
    weight_row = iota((rows, LANE), 0)
    weights = []
    for b in range(blocks):
        weight = jnp.zeros((rows, LANE), jnp.float32)
        for l in range(rows):
            weight = jnp.where(weight_row == l, w_smem[b * rows + l], weight)
        weights.append(weight)
    side = sources * n
    order_i = iota((side, side), 0)
    by_device = one_hot(iota((side, side), 1) == lax.rem(order_i, sources) * n + lax.div(order_i, sources))

    def send_waves(u):
        got = z_recv.at[u, 0 : sources - 1]
        remote(got, got, zs_sem.at[u], zr_sem.at[u], (x, y, z, c)).wait_recv()
        w_recv_own = w_recv.at[u, me_first]
        for b in range(blocks):
            tiles = jnp.dot(by_device, z_recv[u, :, b].reshape(side, LANE), preferred_element_type=jnp.float32)
            tiles = lanes_for_rows(tiles.reshape(n * sides, rows, LANE), rows, width)
            w_send[u, :, :, b] = (tiles * weights[b][None]).astype(jnp.bfloat16).reshape(n, sides, rows, LANE)
            if b + 1 not in (blocks // 2 + 1, blocks):
                continue
            at = slice(0, b + 1) if b + 1 < blocks else slice(blocks // 2 + 1, blocks)
            w_recv_own[:, at] = w_send[u, me_first, :, at]
            for r in far_first:
                t = wrap(me_first + r)
                remote(
                    w_send.at[u, t, :, at], w_recv_own.at[:, at], ws_sem.at[u], wr_sem.at[u], first_axis(t)
                ).start()

    def wait_waves(u):
        got = w_recv.at[u, 0 : n - 1]
        remote(got, got, ws_sem.at[u], wr_sem.at[u], (x, y, z, c)).wait_recv()

    send_waves(0)

    @pl.when(c == 1)
    def _():
        send_waves(1)

    got = t_recv.at[0 : n - 1]
    remote(got, got, ts_sem, tr_sem, (x, y, z, c)).wait_recv()
    wait_waves(0)

    depth_all = n * lats
    pair_id = pair_smem[jnp.where(c == 0, x * n + z, z * n + y)]
    limit = TRUNC - SPACING * pair_id - SPACING // 2

    def waves_of(u):
        return jnp.concatenate([w_recv[u, :, s].reshape(depth_all, LANE) for s in range(sides)], axis=1)

    def table_of(j0, j1):
        return t_recv[:, :, :, j0 * LANE : j1 * LANE].reshape(depth_all, (j1 - j0) * LANE)

    all_spans = [(k, min(k + 2, j1)) for j0, j1 in PIECES for k in range(j0, j1, 2)]

    def sums_of(waves, k0, k1):
        return tn(waves, table_of(k0, k1)).reshape(n, 2 * ch, (k1 - k0) * LANE)

    low_waves = waves_of(0)
    for k0, k1 in all_spans:
        part[:, :, k0 * LANE : k1 * LANE] = sums_of(low_waves, k0, k1)

    @pl.when(c == 1)
    def _():
        wait_waves(1)

    def product_high(j0, j1):
        @pl.when(c == 1)
        def _():
            high_waves = waves_of(1)
            for k0, k1 in all_spans:
                if j0 <= k0 < j1:
                    at = slice(k0 * LANE, k1 * LANE)
                    column = half + k0 * LANE + iota((n, 2 * ch, (k1 - k0) * LANE), 2)
                    part[:, :, at] = jnp.where(column < limit, part[:, :, at], sums_of(high_waves, k0, k1))

    def up(k):
        return wrap(me_second + k)

    far = n == 8
    ways = ((1, -1), (0, 1)) if far else ((0, 1),)
    stage, near, late = {}, {}, {}

    def span_of(p):
        return slice(PIECES[p][0] * LANE, PIECES[p][1] * LANE)

    def send_far(p):
        at = span_of(p)
        for i, sign in ways if far else ():
            stage[p, i] = (
                remote(
                    part.at[up(3 * sign), :, at], a3.at[i, :, at], a_ssem.at[p, i], a_rsem.at[p, i],
                    second_axis(up(sign)),
                ),
                remote(
                    part.at[up(4), i * ch : (i + 1) * ch, at], a4.at[i, :, at], a_ssem.at[p, 2 + i],
                    a_rsem.at[p, 2 + i], second_axis(up(2 * sign)),
                ),
            )
            for send in stage[p, i]:
                send.start()

    def send_near(p):
        at = span_of(p)
        for i, sign in ways:
            near[p, i] = remote(
                part.at[up(sign), :, at], fin.at[i, :, at], f_ssem.at[p, i], f_rsem.at[p, i], second_axis(up(sign))
            )
            near[p, i].start()

    def merge(p):
        at = span_of(p)
        for i, sign in ways if far else ():
            stage[p, i][0].wait_recv()
            merged[i, :, at] = part[up(2 * sign), :, at] + a3[i, :, at]
            stage[p, i][1].wait_recv()
            mine = slice(i * ch, (i + 1) * ch)
            merged[i, mine, at] = merged[i, mine, at] + a4[i, :, at]
            late[p, i] = remote(
                merged.at[i, :, at], fin.at[2 + i, :, at], f_ssem.at[p, 2 + i], f_rsem.at[p, 2 + i],
                second_axis(up(2 * sign)),
            )
            late[p, i].start()

    def final(p):
        at = span_of(p)
        total = part[me_second, :, at]
        for i, _ in ways:
            near[p, i].wait_recv()
            total = total + fin[i, :, at]
        for i, _ in ways if far else ():
            late[p, i].wait_recv()
            total = total + fin[2 + i, :, at]
        return total

    product_high(*PIECES[0])
    send_far(0)
    product_high(*PIECES[1])
    send_far(1)
    send_near(0)
    merge(0)
    merge(1)
    send_near(1)
    total = jnp.concatenate([final(0), final(1)], axis=1)

    levels = sources * ch // 2
    channel = me_second * 2 * ch + iota((2 * ch, LANE), 0)
    factor = 1.0 + 2.0 * lax.shift_right_logical(channel, 1).astype(jnp.float32) / (levels - 1)
    squares = None
    for j in range(chunks):
        column = total[:, j * LANE : (j + 1) * LANE]
        squares = column * column if squares is None else squares + column * column
    squares = factor * squares
    tile = squares[0:8]
    for i in range(1, 2 * ch // 8):
        tile = tile + squares[i * 8 : i * 8 + 8]

    def share(ref, at, tile, sem, devices):
        ref[at] = tile
        for device in devices:
            remote(ref.at[at], ref.at[at], e_ssem.at[sem], e_rsem.at[sem], device).start()

    def added(ref, size, sem):
        got = ref.at[0 : size - 1]
        remote(got, got, e_ssem.at[sem], e_rsem.at[sem], (x, y, z, c)).wait_recv()
        tile = ref[0]
        for i in range(1, size):
            tile = tile + ref[i]
        return tile

    peers = [(x, y, wrap(z + r), k) for r in far_first for k in (c, other)] + [(x, y, z, other)]
    share(e0, me, tile, 0, peers)
    total_ref[...] = total

    tile = added(e0, sources, 0)
    at_home = jnp.where(c == 0, y, x) == z

    def rows_of(core):
        return total_ref.at[pl.ds(pl.multiple_of(core * ch, 8), ch)]

    home = out_hbm.at[:, pl.ds(pl.multiple_of(c * half, LANE), half)]
    at_home_copy = pltpu.make_async_copy(rows_of(c), home, load_sem.at[5])

    def to_owner(core):
        device = (jnp.where(c == 0, x, z), jnp.where(c == 0, z, y), me_second, core)
        return remote(rows_of(core), home, o_ssem.at[core], o_rsem.at[c], device)

    to_owner(other).start()

    @pl.when(at_home)
    def _():
        at_home_copy.start()

    @pl.when(jnp.logical_not(at_home))
    def _():
        to_owner(c).start()

    tile = jnp.sum(tile, axis=0, keepdims=True)
    ring = [min(r, n - r) for r in range(n)]
    steps = sorted(((i, j) for i in range(n) for j in range(n) if i or j), key=lambda s: -ring[s[0]] - ring[s[1]])
    e_row[...] = tile
    e_own = e1_hbm.at[x * n + y]
    for i, j in steps:
        remote(e_row, e_own, e_ssem.at[1], e_rsem.at[1], (wrap(x + i), wrap(y + j), z, c)).start()
    e_copy = pltpu.make_async_copy(e_row, e_own, load_sem.at[6])
    e_copy.start()

    got = e1_hbm.at[0 : pairs - 1]
    remote(got, got, e_ssem.at[1], e_rsem.at[1], (x, y, z, c)).wait_recv()
    e_copy.wait()

    def from_core(core):
        got = out_hbm.at[:, pl.ds(pl.multiple_of(core * half, LANE), half)]
        return remote(got, got, o_ssem.at[core], o_rsem.at[core], (x, y, z, c))

    from_core(other).wait_recv()

    @pl.when(at_home)
    def _():
        at_home_copy.wait()

    @pl.when(jnp.logical_not(at_home))
    def _():
        from_core(c).wait_recv()

    first = z_recv.at[0, 0 : sources - 1]
    remote(first, first, zs_sem.at[0], zr_sem.at[0], (x, y, z, c)).wait_send()

    @pl.when(c == 0)
    def _():
        second = z_recv.at[1, 0:n]
        remote(second, second, zs_sem.at[1], zr_sem.at[1], (x, y, z, c)).wait_send()

    @pl.when(c == 1)
    def _():
        second = z_recv.at[1, 0 : n - 1]
        remote(second, second, zs_sem.at[1], zr_sem.at[1], (x, y, z, c)).wait_send()
        gone = w_send.at[1, 0 : n - 1]
        remote(gone, gone, ws_sem.at[1], wr_sem.at[1], (x, y, z, c)).wait_send()

    gone = w_send.at[0, 0 : n - 1]
    remote(gone, gone, ws_sem.at[0], wr_sem.at[0], (x, y, z, c)).wait_send()
    gone = t_send.at[0 : n - 1]
    remote(gone, gone, ts_sem, tr_sem, (x, y, z, c)).wait_send()
    for key in near:
        near[key].wait_send()
    for key in late:
        stage[key][0].wait_send()
        stage[key][1].wait_send()
        late[key].wait_send()
    to_owner(other).wait_send()

    @pl.when(jnp.logical_not(at_home))
    def _():
        to_owner(c).wait_send()

    for sem, ref, size in ((0, e0, sources), (1, e1_hbm, pairs)):
        gone = ref.at[0 : size - 1]
        remote(gone, gone, e_ssem.at[sem], e_rsem.at[sem], (x, y, z, c)).wait_send()


def outputs_kernel(scale, block_hbm, rows_hbm, out_hbm, energy_ref, block, rows, sem):
    loads = [pltpu.make_async_copy(block_hbm, block, sem.at[0]), pltpu.make_async_copy(rows_hbm, rows, sem.at[1])]
    for load in loads:
        load.start()
    loads[0].wait()
    store = pltpu.make_async_copy(block, out_hbm, sem.at[2])
    store.start()
    loads[1].wait()
    energy_ref[0, 0] = jnp.sum(jnp.sum(rows[...], axis=0)) * scale
    store.wait()


def shards(n, fourier, quad_weights, legendre, owner_pair):
    ch, lats, _ = fourier.shape
    _, pairs, length = legendre.shape
    half = length // 2
    rows = LANE // ch
    blocks = lats // rows
    sides = 2 * n // rows
    bf16, f32 = jnp.bfloat16, jnp.float32
    vmem, dma = pltpu.VMEM, pltpu.SemaphoreType.DMA
    hbm = pl.BlockSpec(memory_space=pltpu.HBM)
    smem = pl.BlockSpec(memory_space=pltpu.SMEM)
    limit = pltpu.CompilerParams(vmem_limit_bytes=67_043_328)
    block, energy_rows = pl.pallas_call(
        functools.partial(kernel, n),
        out_shape=(
            jax.ShapeDtypeStruct((ch, length), f32),
            jax.ShapeDtypeStruct((pairs, 1, LANE), f32),
        ),
        in_specs=[hbm] * 5,
        out_specs=(hbm, hbm),
        scratch_shapes=[
            vmem((ch, lats, M_WIN), bf16),
            vmem((ch * lats, M_WIN), f32),
            vmem((blocks, LANE, M_WIN), bf16),
            vmem((lats, pairs, half), bf16),
            vmem((1, pairs), jnp.int32),
            pltpu.SMEM((pairs,), jnp.int32),
            pltpu.SMEM((lats,), f32),
            vmem((3, n, blocks, n, LANE), bf16),
            vmem((2, 2 * n, blocks, n, LANE), bf16),
            vmem((2, n, sides, blocks, rows, LANE), bf16),
            vmem((2, n, sides, blocks, rows, LANE), bf16),
            vmem((n, blocks, rows, half), bf16),
            vmem((n, blocks, rows, half), bf16),
            vmem((n, 2 * ch, half), f32),
            vmem((2, 2 * ch, half), f32),
            vmem((2, ch, half), f32),
            vmem((2, 2 * ch, half), f32),
            vmem((4, 2 * ch, half), f32),
            vmem((2 * ch, half), f32),
            vmem((2 * n, 8, LANE), f32),
            vmem((1, LANE), f32),
            dma((7,)),
            dma((2,)),
            dma((2,)),
            dma((2,)),
            dma((2,)),
            dma,
            dma,
            dma((2, 4)),
            dma((2, 4)),
            dma((2, 4)),
            dma((2, 4)),
            dma((2,)),
            dma((2,)),
            dma((2,)),
            dma((2,)),
        ],
        compiler_params=pltpu.CompilerParams(collective_id=0, has_side_effects=True, vmem_limit_bytes=67_043_328),
        name="legendre",
    )(fourier, quad_weights, legendre, owner_pair.reshape(1, pairs), owner_pair)
    spectra, energy = pl.pallas_call(
        functools.partial(outputs_kernel, 1.0 / (pairs * 2 * n * ch * length)),
        out_shape=(
            jax.ShapeDtypeStruct((ch, length), f32),
            jax.ShapeDtypeStruct((1, 1), f32),
        ),
        in_specs=[hbm] * 2,
        out_specs=(hbm, smem),
        scratch_shapes=[vmem((ch, length), f32), vmem((pairs, 1, LANE), f32), dma((3,))],
        compiler_params=limit,
        name="outputs",
    )(block, energy_rows)
    return spectra[None], energy[0, 0]


def solution(mesh):
    n = mesh.shape["lev"] // 2
    finer = Mesh(mesh.devices.reshape(n, n, n, 2), LAT + LEV)
    return jax.shard_map(
        functools.partial(shards, n),
        mesh=finer,
        in_specs=(P(LEV, LAT, None), P(LAT), P(LAT, None, None), P()),
        out_specs=(P(LAT, LEV, None), P()),
        check_vma=False,
    )
```

```python
import functools

import jax
import jax.numpy as jnp
from jax import lax
from jax.experimental import pallas as pl
from jax.experimental.pallas import tpu as pltpu
from jax.sharding import Mesh
from jax.sharding import PartitionSpec as P

MESH = pl.DeviceIdType.MESH
TRUNC = 1280
M_WIN = 128
SPACING = 10
LAT = ("lat_0", "lat_1")
LEV = ("lev_0", "lev_1")
LANE = 128
PIECES = ((0, 3), (3, 5))


def nt(a, b):
    return lax.dot_general(a, b, (((1,), (1,)), ((), ())), preferred_element_type=jnp.float32)


def one_hot(condition):
    return jnp.where(condition, 1.0, 0.0).astype(jnp.bfloat16)


def iota(shape, dim):
    return lax.broadcasted_iota(jnp.int32, shape, dim)


def lanes_for_rows(tiles, paired, rows, width):
    row, lane = iota(tiles.shape, 1), iota(tiles.shape, 2)
    group = lax.div(lane, width)
    step = 1
    while step < rows:
        row_bit, group_bit = lax.rem(lax.div(row, step), 2), lax.rem(lax.div(group, step), 2)
        swapped_up = paired if step == 1 else pltpu.roll(tiles, rows - step, 1)
        moved = pltpu.roll(swapped_up, step * width, 2)
        if 2 * step < rows:
            swapped_down = paired if step == 1 else pltpu.roll(tiles, step, 1)
            moved = jnp.where(row_bit > group_bit, pltpu.roll(swapped_down, LANE - step * width, 2), moved)
        tiles = jnp.where(row_bit == group_bit, tiles, moved)
        step *= 2
    return tiles


def kernel(n, f_hbm, w_hbm, leg_hbm, pair_row_hbm, pair_hbm, out_hbm, e1_hbm,
           f_in, f_rows, g, tin, pair_row, pair_smem, w_smem, z_send, z_recv, w_send, w_recv, w_turned, t_send, t_recv,
           part, a3, a4, merged, fin, total_ref, e0, e_row,
           load_sem, zs_sem, zr_sem, ws_sem, wr_sem, ts_sem, tr_sem,
           a_ssem, a_rsem, f_ssem, f_rsem, o_ssem, o_rsem, e_ssem, e_rsem):
    x, y, z, c = (lax.axis_index(a) for a in LAT + LEV)
    ch, lats, _ = f_in.shape
    half = tin.shape[2]
    chunks = half // LANE
    other = 1 - c
    pairs = n * n
    sources = 2 * n
    width = ch
    rows = LANE // width
    blocks = lats // rows
    sides = sources // rows
    me = z * 2 + c

    def first_axis(j):
        return (jnp.where(c == 0, j, x), jnp.where(c == 0, y, j), z, c)

    def second_axis(j):
        return (jnp.where(c == 0, x, j), jnp.where(c == 0, j, y), z, c)

    me_first = jnp.where(c == 0, x, y)
    me_second = jnp.where(c == 0, y, x)

    def wrap(v):
        return lax.rem(v + n, n)

    loads = [
        pltpu.make_async_copy(f_hbm, f_in, load_sem.at[0]),
        pltpu.make_async_copy(pair_row_hbm, pair_row, load_sem.at[1]),
        pltpu.make_async_copy(w_hbm, w_smem, load_sem.at[2]),
        pltpu.make_async_copy(leg_hbm.at[:, :, pl.ds(pl.multiple_of(c * half, LANE), half)], tin, load_sem.at[3]),
        pltpu.make_async_copy(pair_hbm, pair_smem, load_sem.at[4]),
    ]
    for load in loads:
        load.start()
    f_load, pair_row_load, w_load, table_load, pair_load = loads

    barrier = pltpu.get_barrier_semaphore()
    count = 0
    far_first = [r for k in range(n // 2, 0, -1) for r in sorted({k, n - k})]
    for r in far_first:
        for device in (
            (wrap(x + r), y, z, c), (x, wrap(y + r), z, c), (x, y, wrap(z + r), c), (x, y, wrap(z + r), other)
        ):
            pl.semaphore_signal(barrier, inc=1, device_id=device, device_id_type=MESH)
            count += 1
    pl.semaphore_signal(barrier, inc=1, device_id=(x, y, z, other), device_id_type=MESH)
    count += 1

    def remote(src, dst, ssem, rsem, device):
        return pltpu.make_async_remote_copy(
            src_ref=src, dst_ref=dst, send_sem=ssem, recv_sem=rsem, device_id=device, device_id_type=MESH
        )

    pair_row_load.wait()
    row_i, col_i = iota((pairs, pairs), 0), iota((pairs, pairs), 1)
    swapped = one_hot(row_i == lax.rem(col_i, n) * n + lax.div(col_i, n))
    wave_i = iota((M_WIN, pairs), 0)
    ids = jnp.broadcast_to(pair_row[...], (M_WIN, pairs))
    low_hot = one_hot(wave_i == ids)
    high_hot = one_hot(M_WIN - 1 - wave_i == ids)
    plain = one_hot(row_i == col_i)
    sel = jnp.concatenate([nt(swapped, low_hot), nt(plain, low_hot), nt(plain, high_hot)], axis=0).astype(jnp.bfloat16)
    f_load.wait()
    f_rows[...] = f_in[...].astype(jnp.float32).reshape(ch * lats, M_WIN)
    for l in range(lats):
        g[l // rows, l % rows * ch : (l % rows + 1) * ch] = f_rows[pl.ds(l, ch, stride=lats), :].astype(jnp.bfloat16)

    for b in range(blocks):
        got = nt(sel, g[b]).astype(jnp.bfloat16)
        z_send[:, :, b] = got.reshape(3, n, n, LANE)
    z_recv[0, me] = z_send[c, z]
    z_recv[1, me] = z_send[2, z]

    pl.semaphore_wait(barrier, count)

    def z_copy(kind, u, t, core):
        remote(z_send.at[kind, t], z_recv.at[u, me], zs_sem.at[u], zr_sem.at[u], (x, y, t, core)).start()

    for core in (0, 1):
        for r in far_first:
            z_copy(core, 0, wrap(z + r), core)
    z_copy(other, 0, z, other)
    for r in far_first:
        z_copy(2, 1, wrap(z + r), 1)

    @pl.when(c == 0)
    def _():
        z_copy(2, 1, z, 1)

    table_rows = n * rows
    device_i = lax.div(iota((table_rows, pairs), 0), rows)
    owner_i = jnp.where(c == 0, device_i * n + z, z * n + device_i)
    owner_of_row = one_hot(iota((table_rows, pairs), 1) == owner_i)
    depth = rows * pairs
    pair_of = lax.rem(iota((depth, pairs), 0), pairs)
    table_hot = one_hot(pair_of == jnp.broadcast_to(pair_row[...], (depth, pairs)))
    same_lat = lax.rem(iota((table_rows, depth), 0), rows) == lax.div(iota((table_rows, depth), 1), pairs)
    pick = jnp.where(same_lat, nt(owner_of_row, table_hot), 0.0).astype(jnp.bfloat16)
    table_load.wait()
    for b in range(blocks):
        block = tin[b * rows : (b + 1) * rows].reshape(depth, half)
        got = jnp.dot(pick, block, preferred_element_type=jnp.float32).astype(jnp.bfloat16)
        t_send[:, b] = got.reshape(n, rows, half)
    t_recv[me_first] = t_send[me_first]
    for r in far_first:
        t = wrap(me_first + r)
        remote(t_send.at[t], t_recv.at[me_first], ts_sem, tr_sem, first_axis(t)).start()

    w_load.wait()
    pair_load.wait()
    weight_row = iota((rows, LANE), 0)
    weights = []
    for b in range(blocks):
        weight = jnp.zeros((rows, LANE), jnp.float32)
        for l in range(rows):
            weight = jnp.where(weight_row == l, w_smem[b * rows + l], weight)
        weights.append(weight)
    side = sources * n
    order_i = iota((2 * side, side), 0)
    source_i = lax.rem(order_i, sources)
    paired_i = source_i + 1 - 2 * lax.rem(source_i, 2)
    source_i = jnp.where(order_i < side, source_i, paired_i)
    by_device = one_hot(iota((2 * side, side), 1) == source_i * n + lax.div(lax.rem(order_i, side), sources))

    def send_waves(u):
        got = z_recv.at[u, 0 : sources - 1]
        remote(got, got, zs_sem.at[u], zr_sem.at[u], (x, y, z, c)).wait_recv()
        w_recv_own = w_recv.at[u, me_first]
        for b in range(blocks):
            tiles = jnp.dot(by_device, z_recv[u, :, b].reshape(side, LANE), preferred_element_type=jnp.float32)
            tiles = tiles.reshape(2, n * sides, rows, LANE)
            tiles = lanes_for_rows(tiles[0], tiles[1], rows, width)
            w_send[u, :, :, b] = (tiles * weights[b][None]).astype(jnp.bfloat16).reshape(n, sides, rows, LANE)
            if b + 1 not in (blocks // 2 + 1, blocks):
                continue
            at = slice(0, b + 1) if b + 1 < blocks else slice(blocks // 2 + 1, blocks)
            w_recv_own[:, at] = w_send[u, me_first, :, at]
            for r in far_first:
                t = wrap(me_first + r)
                remote(
                    w_send.at[u, t, :, at], w_recv_own.at[:, at], ws_sem.at[u], wr_sem.at[u], first_axis(t)
                ).start()

    def wait_waves(u):
        got = w_recv.at[u, 0 : n - 1]
        remote(got, got, ws_sem.at[u], wr_sem.at[u], (x, y, z, c)).wait_recv()

    send_waves(0)

    @pl.when(c == 1)
    def _():
        send_waves(1)

    got = t_recv.at[0 : n - 1]
    remote(got, got, ts_sem, tr_sem, (x, y, z, c)).wait_recv()
    wait_waves(0)

    depth_all = n * lats
    pair_id = pair_smem[jnp.where(c == 0, x * n + z, z * n + y)]
    limit = TRUNC - SPACING * pair_id - SPACING // 2

    def turn_waves(u):
        for s in range(sides):
            w_turned[u, s * LANE : (s + 1) * LANE] = w_recv[u, :, s].reshape(depth_all, LANE).T

    def table_of(j0, j1):
        return t_recv[:, :, :, j0 * LANE : j1 * LANE].reshape(depth_all, (j1 - j0) * LANE)

    all_spans = [(k, min(k + 2, j1)) for j0, j1 in PIECES for k in range(j0, j1, 2)]

    def sums_of(u, k0, k1):
        sums = jnp.dot(w_turned[u], table_of(k0, k1), preferred_element_type=jnp.float32)
        return sums.reshape(n, 2 * ch, (k1 - k0) * LANE)

    turn_waves(0)
    for k0, k1 in all_spans:
        part[:, :, k0 * LANE : k1 * LANE] = sums_of(0, k0, k1)

    @pl.when(c == 1)
    def _():
        wait_waves(1)
        turn_waves(1)

    def product_high(j0, j1):
        @pl.when(c == 1)
        def _():
            for k0, k1 in all_spans:
                if j0 <= k0 < j1:
                    at = slice(k0 * LANE, k1 * LANE)
                    column = half + k0 * LANE + iota((n, 2 * ch, (k1 - k0) * LANE), 2)
                    part[:, :, at] = jnp.where(column < limit, part[:, :, at], sums_of(1, k0, k1))

    def up(k):
        return wrap(me_second + k)

    far = n == 8
    ways = ((1, -1), (0, 1)) if far else ((0, 1),)
    stage, near, late = {}, {}, {}

    def span_of(p):
        return slice(PIECES[p][0] * LANE, PIECES[p][1] * LANE)

    def send_far(p):
        at = span_of(p)
        for i, sign in ways if far else ():
            stage[p, i] = (
                remote(
                    part.at[up(3 * sign), :, at], a3.at[i, :, at], a_ssem.at[p, i], a_rsem.at[p, i],
                    second_axis(up(sign)),
                ),
                remote(
                    part.at[up(4), i * ch : (i + 1) * ch, at], a4.at[i, :, at], a_ssem.at[p, 2 + i],
                    a_rsem.at[p, 2 + i], second_axis(up(2 * sign)),
                ),
            )
            for send in stage[p, i]:
                send.start()

    def send_near(p):
        at = span_of(p)
        for i, sign in ways:
            near[p, i] = remote(
                part.at[up(sign), :, at], fin.at[i, :, at], f_ssem.at[p, i], f_rsem.at[p, i], second_axis(up(sign))
            )
            near[p, i].start()

    def merge(p):
        at = span_of(p)
        for i, sign in ways if far else ():
            stage[p, i][0].wait_recv()
            merged[i, :, at] = part[up(2 * sign), :, at] + a3[i, :, at]
            stage[p, i][1].wait_recv()
            mine = slice(i * ch, (i + 1) * ch)
            merged[i, mine, at] = merged[i, mine, at] + a4[i, :, at]
            late[p, i] = remote(
                merged.at[i, :, at], fin.at[2 + i, :, at], f_ssem.at[p, 2 + i], f_rsem.at[p, 2 + i],
                second_axis(up(2 * sign)),
            )
            late[p, i].start()

    def final(p):
        at = span_of(p)
        total = part[me_second, :, at]
        for i, _ in ways:
            near[p, i].wait_recv()
            total = total + fin[i, :, at]
        for i, _ in ways if far else ():
            late[p, i].wait_recv()
            total = total + fin[2 + i, :, at]
        return total

    product_high(*PIECES[0])
    send_far(0)
    product_high(*PIECES[1])
    send_far(1)
    send_near(0)
    merge(0)
    merge(1)
    send_near(1)
    total = jnp.concatenate([final(0), final(1)], axis=1)

    levels = sources * ch // 2
    channel = me_second * 2 * ch + iota((2 * ch, LANE), 0)
    factor = 1.0 + 2.0 * lax.shift_right_logical(channel, 1).astype(jnp.float32) / (levels - 1)
    squares = None
    for j in range(chunks):
        column = total[:, j * LANE : (j + 1) * LANE]
        squares = column * column if squares is None else squares + column * column
    squares = factor * squares
    tile = squares[0:8]
    for i in range(1, 2 * ch // 8):
        tile = tile + squares[i * 8 : i * 8 + 8]

    def share(ref, at, tile, sem, devices):
        ref[at] = tile
        for device in devices:
            remote(ref.at[at], ref.at[at], e_ssem.at[sem], e_rsem.at[sem], device).start()

    def added(ref, size, sem):
        got = ref.at[0 : size - 1]
        remote(got, got, e_ssem.at[sem], e_rsem.at[sem], (x, y, z, c)).wait_recv()
        tile = ref[0]
        for i in range(1, size):
            tile = tile + ref[i]
        return tile

    peers = [(x, y, wrap(z + r), k) for r in far_first for k in (c, other)] + [(x, y, z, other)]
    share(e0, me, tile, 0, peers)
    total_ref[...] = total

    tile = added(e0, sources, 0)
    at_home = jnp.where(c == 0, y, x) == z

    def rows_of(core):
        return total_ref.at[pl.ds(pl.multiple_of(core * ch, 8), ch)]

    home = out_hbm.at[:, pl.ds(pl.multiple_of(c * half, LANE), half)]
    at_home_copy = pltpu.make_async_copy(rows_of(c), home, load_sem.at[5])

    def to_owner(core):
        device = (jnp.where(c == 0, x, z), jnp.where(c == 0, z, y), me_second, core)
        return remote(rows_of(core), home, o_ssem.at[core], o_rsem.at[c], device)

    to_owner(other).start()

    @pl.when(at_home)
    def _():
        at_home_copy.start()

    @pl.when(jnp.logical_not(at_home))
    def _():
        to_owner(c).start()

    tile = jnp.sum(tile, axis=0, keepdims=True)
    ring = [min(r, n - r) for r in range(n)]
    steps = sorted(((i, j) for i in range(n) for j in range(n) if i or j), key=lambda s: -ring[s[0]] - ring[s[1]])
    e_row[...] = tile
    e_own = e1_hbm.at[x * n + y]
    for i, j in steps:
        remote(e_row, e_own, e_ssem.at[1], e_rsem.at[1], (wrap(x + i), wrap(y + j), z, c)).start()
    e_copy = pltpu.make_async_copy(e_row, e_own, load_sem.at[6])
    e_copy.start()

    got = e1_hbm.at[0 : pairs - 1]
    remote(got, got, e_ssem.at[1], e_rsem.at[1], (x, y, z, c)).wait_recv()
    e_copy.wait()

    def from_core(core):
        got = out_hbm.at[:, pl.ds(pl.multiple_of(core * half, LANE), half)]
        return remote(got, got, o_ssem.at[core], o_rsem.at[core], (x, y, z, c))

    from_core(other).wait_recv()

    @pl.when(at_home)
    def _():
        at_home_copy.wait()

    @pl.when(jnp.logical_not(at_home))
    def _():
        from_core(c).wait_recv()

    first = z_recv.at[0, 0 : sources - 1]
    remote(first, first, zs_sem.at[0], zr_sem.at[0], (x, y, z, c)).wait_send()

    @pl.when(c == 0)
    def _():
        second = z_recv.at[1, 0:n]
        remote(second, second, zs_sem.at[1], zr_sem.at[1], (x, y, z, c)).wait_send()

    @pl.when(c == 1)
    def _():
        second = z_recv.at[1, 0 : n - 1]
        remote(second, second, zs_sem.at[1], zr_sem.at[1], (x, y, z, c)).wait_send()
        gone = w_send.at[1, 0 : n - 1]
        remote(gone, gone, ws_sem.at[1], wr_sem.at[1], (x, y, z, c)).wait_send()

    gone = w_send.at[0, 0 : n - 1]
    remote(gone, gone, ws_sem.at[0], wr_sem.at[0], (x, y, z, c)).wait_send()
    gone = t_send.at[0 : n - 1]
    remote(gone, gone, ts_sem, tr_sem, (x, y, z, c)).wait_send()
    for key in near:
        near[key].wait_send()
    for key in late:
        stage[key][0].wait_send()
        stage[key][1].wait_send()
        late[key].wait_send()
    to_owner(other).wait_send()

    @pl.when(jnp.logical_not(at_home))
    def _():
        to_owner(c).wait_send()

    for sem, ref, size in ((0, e0, sources), (1, e1_hbm, pairs)):
        gone = ref.at[0 : size - 1]
        remote(gone, gone, e_ssem.at[sem], e_rsem.at[sem], (x, y, z, c)).wait_send()


def outputs_kernel(scale, block_hbm, rows_hbm, out_hbm, energy_hbm, block, rows, energy, sem):
    loads = [pltpu.make_async_copy(rows_hbm, rows, sem.at[0]), pltpu.make_async_copy(block_hbm, block, sem.at[1])]
    stores = [pltpu.make_async_copy(energy, energy_hbm, sem.at[2]), pltpu.make_async_copy(block, out_hbm, sem.at[3])]
    for load in loads:
        load.start()
    loads[1].wait()
    stores[1].start()
    loads[0].wait()
    energy[0, 0] = jnp.sum(jnp.sum(rows[...], axis=0)) * scale
    stores[0].start()
    for store in stores:
        store.wait()


def shards(n, fourier, quad_weights, legendre, owner_pair):
    ch, lats, _ = fourier.shape
    _, pairs, length = legendre.shape
    half = length // 2
    rows = LANE // ch
    blocks = lats // rows
    sides = 2 * n // rows
    bf16, f32 = jnp.bfloat16, jnp.float32
    vmem, dma = pltpu.VMEM, pltpu.SemaphoreType.DMA
    hbm = pl.BlockSpec(memory_space=pltpu.HBM)
    limit = pltpu.CompilerParams(vmem_limit_bytes=67_043_328)
    block, energy_rows = pl.pallas_call(
        functools.partial(kernel, n),
        out_shape=(
            jax.ShapeDtypeStruct((ch, length), f32),
            jax.ShapeDtypeStruct((pairs, 1, LANE), f32),
        ),
        in_specs=[hbm] * 5,
        out_specs=(hbm, hbm),
        scratch_shapes=[
            vmem((ch, lats, M_WIN), bf16),
            vmem((ch * lats, M_WIN), f32),
            vmem((blocks, LANE, M_WIN), bf16),
            vmem((lats, pairs, half), bf16),
            vmem((1, pairs), jnp.int32),
            pltpu.SMEM((pairs,), jnp.int32),
            pltpu.SMEM((lats,), f32),
            vmem((3, n, blocks, n, LANE), bf16),
            vmem((2, 2 * n, blocks, n, LANE), bf16),
            vmem((2, n, sides, blocks, rows, LANE), bf16),
            vmem((2, n, sides, blocks, rows, LANE), bf16),
            vmem((2, 2 * n * ch, n * lats), bf16),
            vmem((n, blocks, rows, half), bf16),
            vmem((n, blocks, rows, half), bf16),
            vmem((n, 2 * ch, half), f32),
            vmem((2, 2 * ch, half), f32),
            vmem((2, ch, half), f32),
            vmem((2, 2 * ch, half), f32),
            vmem((4, 2 * ch, half), f32),
            vmem((2 * ch, half), f32),
            vmem((2 * n, 8, LANE), f32),
            vmem((1, LANE), f32),
            dma((7,)),
            dma((2,)),
            dma((2,)),
            dma((2,)),
            dma((2,)),
            dma,
            dma,
            dma((2, 4)),
            dma((2, 4)),
            dma((2, 4)),
            dma((2, 4)),
            dma((2,)),
            dma((2,)),
            dma((2,)),
            dma((2,)),
        ],
        compiler_params=pltpu.CompilerParams(collective_id=0, has_side_effects=True, vmem_limit_bytes=67_043_328),
        name="legendre",
    )(fourier, quad_weights, legendre, owner_pair.reshape(1, pairs), owner_pair)
    spectra, energy = pl.pallas_call(
        functools.partial(outputs_kernel, 1.0 / (pairs * 2 * n * ch * length)),
        out_shape=(
            jax.ShapeDtypeStruct((ch, length), f32),
            jax.ShapeDtypeStruct((1, 1), f32),
        ),
        in_specs=[hbm] * 2,
        out_specs=(hbm, hbm),
        scratch_shapes=[vmem((ch, length), f32), vmem((pairs, 1, LANE), f32), pltpu.SMEM((1, 1), f32), dma((4,))],
        compiler_params=limit,
        name="outputs",
    )(block, energy_rows)
    return spectra[None], energy[0, 0]


def solution(mesh):
    n = mesh.shape["lev"] // 2
    finer = Mesh(mesh.devices.reshape(n, n, n, 2), LAT + LEV)
    return jax.shard_map(
        functools.partial(shards, n),
        mesh=finer,
        in_specs=(P(LEV, LAT, None), P(LAT), P(LAT, None, None), P()),
        out_specs=(P(LAT, LEV, None), P()),
        check_vma=False,
    )
```

```python
import functools

import jax
import jax.numpy as jnp
from jax import lax
from jax.experimental import pallas as pl
from jax.experimental.pallas import tpu as pltpu
from jax.sharding import Mesh
from jax.sharding import PartitionSpec as P

MESH = pl.DeviceIdType.MESH
TRUNC = 1280
M_WIN = 128
SPACING = 10
LAT = ("lat_0", "lat_1")
LEV = ("lev_0", "lev_1")
LANE = 128
PIECES = ((0, 3), (3, 5))


def nt(a, b):
    return lax.dot_general(a, b, (((1,), (1,)), ((), ())), preferred_element_type=jnp.float32)


def one_hot(condition):
    return jnp.where(condition, 1.0, 0.0).astype(jnp.bfloat16)


def iota(shape, dim):
    return lax.broadcasted_iota(jnp.int32, shape, dim)


def lanes_for_rows(tiles, paired, rows, width):
    row, lane = iota(tiles.shape, 1), iota(tiles.shape, 2)
    group = lax.div(lane, width)
    step = 1
    while step < rows:
        row_bit, group_bit = lax.rem(lax.div(row, step), 2), lax.rem(lax.div(group, step), 2)
        swapped_up = paired if step == 1 else pltpu.roll(tiles, rows - step, 1)
        moved = pltpu.roll(swapped_up, step * width, 2)
        if 2 * step < rows:
            swapped_down = paired if step == 1 else pltpu.roll(tiles, step, 1)
            moved = jnp.where(row_bit > group_bit, pltpu.roll(swapped_down, LANE - step * width, 2), moved)
        tiles = jnp.where(row_bit == group_bit, tiles, moved)
        step *= 2
    return tiles


def kernel(n, f_hbm, w_hbm, leg_hbm, pair_row_hbm, pair_hbm, out_hbm, e1_hbm,
           f_in, f_rows, g, tin, pair_row, pair_smem, w_smem, z_send, z_recv, w_send, w_recv, w_turned, t_send, t_recv,
           part, a3, a4, merged, fin, total_ref, e0, e_row,
           load_sem, zs_sem, zr_sem, ws_sem, wr_sem, ts_sem, tr_sem,
           a_ssem, a_rsem, f_ssem, f_rsem, o_ssem, o_rsem, e_ssem, e_rsem):
    x, y, z, c = (lax.axis_index(a) for a in LAT + LEV)
    ch, lats, _ = f_in.shape
    half = tin.shape[2]
    chunks = half // LANE
    other = 1 - c
    pairs = n * n
    sources = 2 * n
    width = ch
    rows = LANE // width
    blocks = lats // rows
    sides = sources // rows
    me = z * 2 + c

    def first_axis(j):
        return (jnp.where(c == 0, j, x), jnp.where(c == 0, y, j), z, c)

    def second_axis(j):
        return (jnp.where(c == 0, x, j), jnp.where(c == 0, j, y), z, c)

    me_first = jnp.where(c == 0, x, y)
    me_second = jnp.where(c == 0, y, x)

    def wrap(v):
        return lax.rem(v + n, n)

    loads = [
        pltpu.make_async_copy(f_hbm, f_in, load_sem.at[0]),
        pltpu.make_async_copy(pair_row_hbm, pair_row, load_sem.at[1]),
        pltpu.make_async_copy(w_hbm, w_smem, load_sem.at[2]),
        pltpu.make_async_copy(leg_hbm.at[:, :, pl.ds(pl.multiple_of(c * half, LANE), half)], tin, load_sem.at[3]),
        pltpu.make_async_copy(pair_hbm, pair_smem, load_sem.at[4]),
    ]
    for load in loads:
        load.start()
    f_load, pair_row_load, w_load, table_load, pair_load = loads

    barrier = pltpu.get_barrier_semaphore()
    count = 0
    far_first = [r for k in range(n // 2, 0, -1) for r in sorted({k, n - k})]
    for r in far_first:
        for device in (
            (wrap(x + r), y, z, c), (x, wrap(y + r), z, c), (x, y, wrap(z + r), c), (x, y, wrap(z + r), other)
        ):
            pl.semaphore_signal(barrier, inc=1, device_id=device, device_id_type=MESH)
            count += 1
    pl.semaphore_signal(barrier, inc=1, device_id=(x, y, z, other), device_id_type=MESH)
    count += 1

    def remote(src, dst, ssem, rsem, device):
        return pltpu.make_async_remote_copy(
            src_ref=src, dst_ref=dst, send_sem=ssem, recv_sem=rsem, device_id=device, device_id_type=MESH
        )

    pair_row_load.wait()
    row_i, col_i = iota((pairs, pairs), 0), iota((pairs, pairs), 1)
    swapped = one_hot(row_i == lax.rem(col_i, n) * n + lax.div(col_i, n))
    wave_i = iota((M_WIN, pairs), 0)
    ids = jnp.broadcast_to(pair_row[...], (M_WIN, pairs))
    low_hot = one_hot(wave_i == ids)
    high_hot = one_hot(M_WIN - 1 - wave_i == ids)
    plain = one_hot(row_i == col_i)
    sel = jnp.concatenate([nt(swapped, low_hot), nt(plain, low_hot), nt(plain, high_hot)], axis=0).astype(jnp.bfloat16)
    f_load.wait()
    f_rows[...] = f_in[...].astype(jnp.float32).reshape(ch * lats, M_WIN)
    for l in range(lats):
        g[l // rows, l % rows * ch : (l % rows + 1) * ch] = f_rows[pl.ds(l, ch, stride=lats), :].astype(jnp.bfloat16)

    for b in range(blocks):
        got = nt(sel, g[b]).astype(jnp.bfloat16)
        z_send[:, :, b] = got.reshape(3, n, n, LANE)
    z_recv[0, me] = z_send[c, z]
    z_recv[1, me] = z_send[2, z]

    pl.semaphore_wait(barrier, count)

    def z_copy(kind, u, t, core):
        remote(z_send.at[kind, t], z_recv.at[u, me], zs_sem.at[u], zr_sem.at[u], (x, y, t, core)).start()

    for core in (0, 1):
        for r in far_first:
            z_copy(core, 0, wrap(z + r), core)
    z_copy(other, 0, z, other)
    for r in far_first:
        z_copy(2, 1, wrap(z + r), 1)

    @pl.when(c == 0)
    def _():
        z_copy(2, 1, z, 1)

    table_rows = n * rows
    device_i = lax.div(iota((table_rows, pairs), 0), rows)
    owner_i = jnp.where(c == 0, device_i * n + z, z * n + device_i)
    owner_of_row = one_hot(iota((table_rows, pairs), 1) == owner_i)
    depth = rows * pairs
    pair_of = lax.rem(iota((depth, pairs), 0), pairs)
    table_hot = one_hot(pair_of == jnp.broadcast_to(pair_row[...], (depth, pairs)))
    same_lat = lax.rem(iota((table_rows, depth), 0), rows) == lax.div(iota((table_rows, depth), 1), pairs)
    pick = jnp.where(same_lat, nt(owner_of_row, table_hot), 0.0).astype(jnp.bfloat16)
    table_load.wait()
    for b in range(blocks):
        block = tin[b * rows : (b + 1) * rows].reshape(depth, half)
        got = jnp.dot(pick, block, preferred_element_type=jnp.float32).astype(jnp.bfloat16)
        t_send[:, b] = got.reshape(n, rows, half)
    t_recv[me_first] = t_send[me_first]
    for r in far_first:
        t = wrap(me_first + r)
        remote(t_send.at[t], t_recv.at[me_first], ts_sem, tr_sem, first_axis(t)).start()

    w_load.wait()
    pair_load.wait()
    weight_row = iota((rows, LANE), 0)
    weights = []
    for b in range(blocks):
        weight = jnp.zeros((rows, LANE), jnp.float32)
        for l in range(rows):
            weight = jnp.where(weight_row == l, w_smem[b * rows + l], weight)
        weights.append(weight)
    side = sources * n
    order_i = iota((2 * side, side), 0)
    source_i = lax.rem(order_i, sources)
    paired_i = source_i + 1 - 2 * lax.rem(source_i, 2)
    source_i = jnp.where(order_i < side, source_i, paired_i)
    by_device = one_hot(iota((2 * side, side), 1) == source_i * n + lax.div(lax.rem(order_i, side), sources))

    def send_waves(u):
        got = z_recv.at[u, 0 : sources - 1]
        remote(got, got, zs_sem.at[u], zr_sem.at[u], (x, y, z, c)).wait_recv()
        w_recv_own = w_recv.at[u, me_first]
        for b in range(blocks):
            tiles = jnp.dot(by_device, z_recv[u, :, b].reshape(side, LANE), preferred_element_type=jnp.float32)
            tiles = tiles.reshape(2, n * sides, rows, LANE)
            tiles = lanes_for_rows(tiles[0], tiles[1], rows, width)
            w_send[u, :, :, b] = (tiles * weights[b][None]).astype(jnp.bfloat16).reshape(n, sides, rows, LANE)
            if b + 1 not in (blocks // 2 + 1, blocks):
                continue
            at = slice(0, b + 1) if b + 1 < blocks else slice(blocks // 2 + 1, blocks)
            w_recv_own[:, at] = w_send[u, me_first, :, at]
            for r in far_first:
                t = wrap(me_first + r)
                remote(
                    w_send.at[u, t, :, at], w_recv_own.at[:, at], ws_sem.at[u], wr_sem.at[u], first_axis(t)
                ).start()

    def wait_waves(u):
        got = w_recv.at[u, 0 : n - 1]
        remote(got, got, ws_sem.at[u], wr_sem.at[u], (x, y, z, c)).wait_recv()

    send_waves(0)

    @pl.when(c == 1)
    def _():
        send_waves(1)

    got = t_recv.at[0 : n - 1]
    remote(got, got, ts_sem, tr_sem, (x, y, z, c)).wait_recv()
    wait_waves(0)

    depth_all = n * lats
    pair_id = pair_smem[jnp.where(c == 0, x * n + z, z * n + y)]
    limit = TRUNC - SPACING * pair_id - SPACING // 2

    def turn_waves(u):
        for s in range(sides):
            w_turned[u, s * LANE : (s + 1) * LANE] = w_recv[u, :, s].reshape(depth_all, LANE).T

    def table_of(j0, j1):
        return t_recv[:, :, :, j0 * LANE : j1 * LANE].reshape(depth_all, (j1 - j0) * LANE)

    all_spans = [(k, min(k + 2, j1)) for j0, j1 in PIECES for k in range(j0, j1, 2)]

    def sums_of(u, k0, k1):
        sums = jnp.dot(w_turned[u], table_of(k0, k1), preferred_element_type=jnp.float32)
        return sums.reshape(n, 2 * ch, (k1 - k0) * LANE)

    turn_waves(0)
    for k0, k1 in all_spans:
        part[:, :, k0 * LANE : k1 * LANE] = sums_of(0, k0, k1)

    @pl.when(c == 1)
    def _():
        wait_waves(1)
        turn_waves(1)

    def product_high(j0, j1):
        @pl.when(c == 1)
        def _():
            for k0, k1 in all_spans:
                if j0 <= k0 < j1:
                    at = slice(k0 * LANE, k1 * LANE)
                    column = half + k0 * LANE + iota((n, 2 * ch, (k1 - k0) * LANE), 2)
                    part[:, :, at] = jnp.where(column < limit, part[:, :, at], sums_of(1, k0, k1))

    def up(k):
        return wrap(me_second + k)

    far = n == 8
    ways = ((1, -1), (0, 1)) if far else ((0, 1),)
    stage, near, late = {}, {}, {}

    def span_of(p):
        return slice(PIECES[p][0] * LANE, PIECES[p][1] * LANE)

    def send_far(p):
        at = span_of(p)
        for i, sign in ways if far else ():
            stage[p, i] = (
                remote(
                    part.at[up(3 * sign), :, at], a3.at[i, :, at], a_ssem.at[p, i], a_rsem.at[p, i],
                    second_axis(up(sign)),
                ),
                remote(
                    part.at[up(4), i * ch : (i + 1) * ch, at], a4.at[i, :, at], a_ssem.at[p, 2 + i],
                    a_rsem.at[p, 2 + i], second_axis(up(2 * sign)),
                ),
            )
            for send in stage[p, i]:
                send.start()

    def send_near(p):
        at = span_of(p)
        for i, sign in ways:
            near[p, i] = remote(
                part.at[up(sign), :, at], fin.at[i, :, at], f_ssem.at[p, i], f_rsem.at[p, i], second_axis(up(sign))
            )
            near[p, i].start()

    def merge(p):
        at = span_of(p)
        for i, sign in ways if far else ():
            stage[p, i][0].wait_recv()
            merged[i, :, at] = part[up(2 * sign), :, at] + a3[i, :, at]
            stage[p, i][1].wait_recv()
            mine = slice(i * ch, (i + 1) * ch)
            merged[i, mine, at] = merged[i, mine, at] + a4[i, :, at]
            late[p, i] = remote(
                merged.at[i, :, at], fin.at[2 + i, :, at], f_ssem.at[p, 2 + i], f_rsem.at[p, 2 + i],
                second_axis(up(2 * sign)),
            )
            late[p, i].start()

    def final(p):
        at = span_of(p)
        total = part[me_second, :, at]
        for i, _ in ways:
            near[p, i].wait_recv()
            total = total + fin[i, :, at]
        for i, _ in ways if far else ():
            late[p, i].wait_recv()
            total = total + fin[2 + i, :, at]
        return total

    product_high(*PIECES[0])
    send_far(0)
    product_high(*PIECES[1])
    send_far(1)
    send_near(0)
    merge(0)
    merge(1)
    send_near(1)
    total = jnp.concatenate([final(0), final(1)], axis=1)

    levels = sources * ch // 2
    channel = me_second * 2 * ch + iota((2 * ch, LANE), 0)
    factor = 1.0 + 2.0 * lax.shift_right_logical(channel, 1).astype(jnp.float32) / (levels - 1)
    squares = None
    for j in range(chunks):
        column = total[:, j * LANE : (j + 1) * LANE]
        squares = column * column if squares is None else squares + column * column
    squares = factor * squares
    tile = squares[0:8]
    for i in range(1, 2 * ch // 8):
        tile = tile + squares[i * 8 : i * 8 + 8]
    tile = jnp.sum(tile, axis=0, keepdims=True)

    def share(ref, at, tile, sem, devices):
        ref[at] = tile
        for device in devices:
            remote(ref.at[at], ref.at[at], e_ssem.at[sem], e_rsem.at[sem], device).start()

    def added(ref, size, sem):
        got = ref.at[0 : size - 1]
        remote(got, got, e_ssem.at[sem], e_rsem.at[sem], (x, y, z, c)).wait_recv()
        tile = ref[0]
        for i in range(1, size):
            tile = tile + ref[i]
        return tile

    peers = [(x, y, wrap(z + r), k) for r in far_first for k in (c, other)] + [(x, y, z, other)]
    share(e0, me, tile, 0, peers)
    total_ref[...] = total

    tile = added(e0, sources, 0)
    at_home = jnp.where(c == 0, y, x) == z

    def rows_of(core):
        return total_ref.at[pl.ds(pl.multiple_of(core * ch, 8), ch)]

    home = out_hbm.at[:, pl.ds(pl.multiple_of(c * half, LANE), half)]
    at_home_copy = pltpu.make_async_copy(rows_of(c), home, load_sem.at[5])

    def to_owner(core):
        device = (jnp.where(c == 0, x, z), jnp.where(c == 0, z, y), me_second, core)
        return remote(rows_of(core), home, o_ssem.at[core], o_rsem.at[c], device)

    ring = [min(r, n - r) for r in range(n)]
    steps = sorted(((i, j) for i in range(n) for j in range(n) if i or j), key=lambda s: -ring[s[0]] - ring[s[1]])
    e_row[...] = tile
    e_own = e1_hbm.at[x * n + y]
    def share_row(steps):
        for i, j in steps:
            remote(e_row, e_own, e_ssem.at[1], e_rsem.at[1], (wrap(x + i), wrap(y + j), z, c)).start()

    far_steps = len(steps) // 3
    share_row(steps[:far_steps])
    to_owner(other).start()

    @pl.when(at_home)
    def _():
        at_home_copy.start()

    @pl.when(jnp.logical_not(at_home))
    def _():
        to_owner(c).start()

    share_row(steps[far_steps:])
    e_copy = pltpu.make_async_copy(e_row, e_own, load_sem.at[6])
    e_copy.start()

    got = e1_hbm.at[0 : pairs - 1]
    remote(got, got, e_ssem.at[1], e_rsem.at[1], (x, y, z, c)).wait_recv()
    e_copy.wait()

    def from_core(core):
        got = out_hbm.at[:, pl.ds(pl.multiple_of(core * half, LANE), half)]
        return remote(got, got, o_ssem.at[core], o_rsem.at[core], (x, y, z, c))

    from_core(other).wait_recv()

    @pl.when(at_home)
    def _():
        at_home_copy.wait()

    @pl.when(jnp.logical_not(at_home))
    def _():
        from_core(c).wait_recv()

    first = z_recv.at[0, 0 : sources - 1]
    remote(first, first, zs_sem.at[0], zr_sem.at[0], (x, y, z, c)).wait_send()

    @pl.when(c == 0)
    def _():
        second = z_recv.at[1, 0:n]
        remote(second, second, zs_sem.at[1], zr_sem.at[1], (x, y, z, c)).wait_send()

    @pl.when(c == 1)
    def _():
        second = z_recv.at[1, 0 : n - 1]
        remote(second, second, zs_sem.at[1], zr_sem.at[1], (x, y, z, c)).wait_send()
        gone = w_send.at[1, 0 : n - 1]
        remote(gone, gone, ws_sem.at[1], wr_sem.at[1], (x, y, z, c)).wait_send()

    gone = w_send.at[0, 0 : n - 1]
    remote(gone, gone, ws_sem.at[0], wr_sem.at[0], (x, y, z, c)).wait_send()
    gone = t_send.at[0 : n - 1]
    remote(gone, gone, ts_sem, tr_sem, (x, y, z, c)).wait_send()
    for key in near:
        near[key].wait_send()
    for key in late:
        stage[key][0].wait_send()
        stage[key][1].wait_send()
        late[key].wait_send()
    to_owner(other).wait_send()

    @pl.when(jnp.logical_not(at_home))
    def _():
        to_owner(c).wait_send()

    for sem, ref, size in ((0, e0, sources), (1, e1_hbm, pairs)):
        gone = ref.at[0 : size - 1]
        remote(gone, gone, e_ssem.at[sem], e_rsem.at[sem], (x, y, z, c)).wait_send()


def outputs_kernel(scale, block_hbm, rows_hbm, out_hbm, energy_hbm, block, rows, energy, sem):
    loads = [pltpu.make_async_copy(rows_hbm, rows, sem.at[0]), pltpu.make_async_copy(block_hbm, block, sem.at[1])]
    stores = [pltpu.make_async_copy(energy, energy_hbm, sem.at[2]), pltpu.make_async_copy(block, out_hbm, sem.at[3])]
    for load in loads:
        load.start()
    loads[1].wait()
    stores[1].start()
    loads[0].wait()
    energy[0, 0] = jnp.sum(jnp.sum(rows[...], axis=0)) * scale
    stores[0].start()
    for store in stores:
        store.wait()


def shards(n, fourier, quad_weights, legendre, owner_pair):
    ch, lats, _ = fourier.shape
    _, pairs, length = legendre.shape
    half = length // 2
    rows = LANE // ch
    blocks = lats // rows
    sides = 2 * n // rows
    bf16, f32 = jnp.bfloat16, jnp.float32
    vmem, dma = pltpu.VMEM, pltpu.SemaphoreType.DMA
    hbm = pl.BlockSpec(memory_space=pltpu.HBM)
    limit = pltpu.CompilerParams(vmem_limit_bytes=67_043_328)
    block, energy_rows = pl.pallas_call(
        functools.partial(kernel, n),
        out_shape=(
            jax.ShapeDtypeStruct((ch, length), f32),
            jax.ShapeDtypeStruct((pairs, 1, LANE), f32),
        ),
        in_specs=[hbm] * 5,
        out_specs=(hbm, hbm),
        scratch_shapes=[
            vmem((ch, lats, M_WIN), bf16),
            vmem((ch * lats, M_WIN), f32),
            vmem((blocks, LANE, M_WIN), bf16),
            vmem((lats, pairs, half), bf16),
            vmem((1, pairs), jnp.int32),
            pltpu.SMEM((pairs,), jnp.int32),
            pltpu.SMEM((lats,), f32),
            vmem((3, n, blocks, n, LANE), bf16),
            vmem((2, 2 * n, blocks, n, LANE), bf16),
            vmem((2, n, sides, blocks, rows, LANE), bf16),
            vmem((2, n, sides, blocks, rows, LANE), bf16),
            vmem((2, 2 * n * ch, n * lats), bf16),
            vmem((n, blocks, rows, half), bf16),
            vmem((n, blocks, rows, half), bf16),
            vmem((n, 2 * ch, half), f32),
            vmem((2, 2 * ch, half), f32),
            vmem((2, ch, half), f32),
            vmem((2, 2 * ch, half), f32),
            vmem((4, 2 * ch, half), f32),
            vmem((2 * ch, half), f32),
            vmem((2 * n, 1, LANE), f32),
            vmem((1, LANE), f32),
            dma((7,)),
            dma((2,)),
            dma((2,)),
            dma((2,)),
            dma((2,)),
            dma,
            dma,
            dma((2, 4)),
            dma((2, 4)),
            dma((2, 4)),
            dma((2, 4)),
            dma((2,)),
            dma((2,)),
            dma((2,)),
            dma((2,)),
        ],
        compiler_params=pltpu.CompilerParams(collective_id=0, has_side_effects=True, vmem_limit_bytes=67_043_328),
        name="legendre",
    )(fourier, quad_weights, legendre, owner_pair.reshape(1, pairs), owner_pair)
    spectra, energy = pl.pallas_call(
        functools.partial(outputs_kernel, 1.0 / (pairs * 2 * n * ch * length)),
        out_shape=(
            jax.ShapeDtypeStruct((ch, length), f32),
            jax.ShapeDtypeStruct((1, 1), f32),
        ),
        in_specs=[hbm] * 2,
        out_specs=(hbm, hbm),
        scratch_shapes=[vmem((ch, length), f32), vmem((pairs, 1, LANE), f32), pltpu.SMEM((1, 1), f32), dma((4,))],
        compiler_params=limit,
        name="outputs",
    )(block, energy_rows)
    return spectra[None], energy[0, 0]


def solution(mesh):
    n = mesh.shape["lev"] // 2
    finer = Mesh(mesh.devices.reshape(n, n, n, 2), LAT + LEV)
    return jax.shard_map(
        functools.partial(shards, n),
        mesh=finer,
        in_specs=(P(LEV, LAT, None), P(LAT), P(LAT, None, None), P()),
        out_specs=(P(LAT, LEV, None), P()),
        check_vma=False,
    )
```

```python
import functools

import jax
import jax.numpy as jnp
from jax import lax
from jax.experimental import pallas as pl
from jax.experimental.pallas import tpu as pltpu
from jax.sharding import Mesh
from jax.sharding import PartitionSpec as P

MESH = pl.DeviceIdType.MESH
TRUNC = 1280
M_WIN = 128
SPACING = 10
LAT = ("lat_0", "lat_1")
LEV = ("lev_0", "lev_1")
LANE = 128
PIECES = ((0, 3), (3, 5))


def nt(a, b):
    return lax.dot_general(a, b, (((1,), (1,)), ((), ())), preferred_element_type=jnp.float32)


def one_hot(condition):
    return jnp.where(condition, 1.0, 0.0).astype(jnp.bfloat16)


def iota(shape, dim):
    return lax.broadcasted_iota(jnp.int32, shape, dim)


def lanes_for_rows(tiles, paired, rows, width):
    row, lane = iota(tiles.shape, 1), iota(tiles.shape, 2)
    group = lax.div(lane, width)
    step = 1
    while step < rows:
        row_bit, group_bit = lax.rem(lax.div(row, step), 2), lax.rem(lax.div(group, step), 2)
        swapped_up = paired if step == 1 else pltpu.roll(tiles, rows - step, 1)
        moved = pltpu.roll(swapped_up, step * width, 2)
        if 2 * step < rows:
            swapped_down = paired if step == 1 else pltpu.roll(tiles, step, 1)
            moved = jnp.where(row_bit > group_bit, pltpu.roll(swapped_down, LANE - step * width, 2), moved)
        tiles = jnp.where(row_bit == group_bit, tiles, moved)
        step *= 2
    return tiles


def kernel(n, f_hbm, w_hbm, leg_hbm, pair_row_hbm, pair_hbm, out_hbm, e1_hbm,
           f_in, f_rows, g, tin, pair_row, pair_smem, w_smem, z_send, z_recv, w_send, w_recv, w_turned, t_send, t_recv,
           part, a3, a4, merged, fin, total_ref, e0, e_row,
           load_sem, zs_sem, zr_sem, ws_sem, wr_sem, ts_sem, tr_sem,
           a_ssem, a_rsem, f_ssem, f_rsem, o_ssem, o_rsem, e_ssem, e_rsem):
    x, y, z, c = (lax.axis_index(a) for a in LAT + LEV)
    ch, lats, _ = f_in.shape
    half = tin.shape[2]
    chunks = half // LANE
    other = 1 - c
    pairs = n * n
    sources = 2 * n
    width = ch
    rows = LANE // width
    blocks = lats // rows
    sides = sources // rows
    me = z * 2 + c

    def first_axis(j):
        return (jnp.where(c == 0, j, x), jnp.where(c == 0, y, j), z, c)

    def second_axis(j):
        return (jnp.where(c == 0, x, j), jnp.where(c == 0, j, y), z, c)

    me_first = jnp.where(c == 0, x, y)
    me_second = jnp.where(c == 0, y, x)

    def wrap(v):
        return lax.rem(v + n, n)

    loads = [
        pltpu.make_async_copy(f_hbm, f_in, load_sem.at[0]),
        pltpu.make_async_copy(pair_row_hbm, pair_row, load_sem.at[1]),
        pltpu.make_async_copy(w_hbm, w_smem, load_sem.at[2]),
        pltpu.make_async_copy(leg_hbm.at[:, :, pl.ds(pl.multiple_of(c * half, LANE), half)], tin, load_sem.at[3]),
        pltpu.make_async_copy(pair_hbm, pair_smem, load_sem.at[4]),
    ]
    for load in loads:
        load.start()
    f_load, pair_row_load, w_load, table_load, pair_load = loads

    barrier = pltpu.get_barrier_semaphore()
    count = 0
    far_first = [r for k in range(n // 2, 0, -1) for r in sorted({k, n - k})]
    for r in far_first:
        for device in (
            (x, y, wrap(z + r), c), (x, y, wrap(z + r), other), (wrap(x + r), y, z, c), (x, wrap(y + r), z, c)
        ):
            pl.semaphore_signal(barrier, inc=1, device_id=device, device_id_type=MESH)
            count += 1
    pl.semaphore_signal(barrier, inc=1, device_id=(x, y, z, other), device_id_type=MESH)
    count += 1

    def remote(src, dst, ssem, rsem, device):
        return pltpu.make_async_remote_copy(
            src_ref=src, dst_ref=dst, send_sem=ssem, recv_sem=rsem, device_id=device, device_id_type=MESH
        )

    pair_row_load.wait()
    row_i, col_i = iota((pairs, pairs), 0), iota((pairs, pairs), 1)
    swapped = one_hot(row_i == lax.rem(col_i, n) * n + lax.div(col_i, n))
    wave_i = iota((M_WIN, pairs), 0)
    ids = jnp.broadcast_to(pair_row[...], (M_WIN, pairs))
    low_hot = one_hot(wave_i == ids)
    high_hot = one_hot(M_WIN - 1 - wave_i == ids)
    plain = one_hot(row_i == col_i)
    sel = jnp.concatenate([nt(swapped, low_hot), nt(plain, low_hot), nt(plain, high_hot)], axis=0).astype(jnp.bfloat16)
    f_load.wait()
    f_rows[...] = f_in[...].astype(jnp.float32).reshape(ch * lats, M_WIN)
    for l in range(lats):
        g[l // rows, l % rows * ch : (l % rows + 1) * ch] = f_rows[pl.ds(l, ch, stride=lats), :].astype(jnp.bfloat16)

    for b in range(blocks):
        got = nt(sel, g[b]).astype(jnp.bfloat16)
        z_send[:, :, b] = got.reshape(3, n, n, LANE)
    z_recv[0, me] = z_send[c, z]
    z_recv[1, me] = z_send[2, z]

    pl.semaphore_wait(barrier, count)

    def z_copy(kind, u, t, core):
        remote(z_send.at[kind, t], z_recv.at[u, me], zs_sem.at[u], zr_sem.at[u], (x, y, t, core)).start()

    for core in (0, 1):
        for r in far_first:
            z_copy(core, 0, wrap(z + r), core)
    z_copy(other, 0, z, other)
    for r in far_first:
        z_copy(2, 1, wrap(z + r), 1)

    @pl.when(c == 0)
    def _():
        z_copy(2, 1, z, 1)

    table_rows = n * rows
    device_i = lax.div(iota((table_rows, pairs), 0), rows)
    owner_i = jnp.where(c == 0, device_i * n + z, z * n + device_i)
    owner_of_row = one_hot(iota((table_rows, pairs), 1) == owner_i)
    depth = rows * pairs
    pair_of = lax.rem(iota((depth, pairs), 0), pairs)
    table_hot = one_hot(pair_of == jnp.broadcast_to(pair_row[...], (depth, pairs)))
    same_lat = lax.rem(iota((table_rows, depth), 0), rows) == lax.div(iota((table_rows, depth), 1), pairs)
    pick = jnp.where(same_lat, nt(owner_of_row, table_hot), 0.0).astype(jnp.bfloat16)
    table_load.wait()
    for b in range(blocks):
        block = tin[b * rows : (b + 1) * rows].reshape(depth, half)
        got = jnp.dot(pick, block, preferred_element_type=jnp.float32).astype(jnp.bfloat16)
        t_send[:, b] = got.reshape(n, rows, half)
    t_recv[me_first] = t_send[me_first]
    for r in far_first:
        t = wrap(me_first + r)
        remote(t_send.at[t], t_recv.at[me_first], ts_sem, tr_sem, first_axis(t)).start()

    w_load.wait()
    pair_load.wait()
    weight_row = iota((rows, LANE), 0)
    weights = []
    for b in range(blocks):
        weight = jnp.zeros((rows, LANE), jnp.float32)
        for l in range(rows):
            weight = jnp.where(weight_row == l, w_smem[b * rows + l], weight)
        weights.append(weight)
    side = sources * n
    order_i = iota((2 * side, side), 0)
    source_i = lax.rem(order_i, sources)
    paired_i = source_i + 1 - 2 * lax.rem(source_i, 2)
    source_i = jnp.where(order_i < side, source_i, paired_i)
    by_device = one_hot(iota((2 * side, side), 1) == source_i * n + lax.div(lax.rem(order_i, side), sources))

    def send_waves(u):
        got = z_recv.at[u, 0 : sources - 1]
        remote(got, got, zs_sem.at[u], zr_sem.at[u], (x, y, z, c)).wait_recv()
        w_recv_own = w_recv.at[u, me_first]
        for b in range(blocks):
            tiles = jnp.dot(by_device, z_recv[u, :, b].reshape(side, LANE), preferred_element_type=jnp.float32)
            tiles = tiles.reshape(2, n * sides, rows, LANE)
            tiles = lanes_for_rows(tiles[0], tiles[1], rows, width)
            w_send[u, :, :, b] = (tiles * weights[b][None]).astype(jnp.bfloat16).reshape(n, sides, rows, LANE)
            if b + 1 not in (blocks // 2 + 1, blocks):
                continue
            at = slice(0, b + 1) if b + 1 < blocks else slice(blocks // 2 + 1, blocks)
            w_recv_own[:, at] = w_send[u, me_first, :, at]
            for r in far_first:
                t = wrap(me_first + r)
                remote(
                    w_send.at[u, t, :, at], w_recv_own.at[:, at], ws_sem.at[u], wr_sem.at[u], first_axis(t)
                ).start()

    def wait_waves(u):
        got = w_recv.at[u, 0 : n - 1]
        remote(got, got, ws_sem.at[u], wr_sem.at[u], (x, y, z, c)).wait_recv()

    send_waves(0)

    @pl.when(c == 1)
    def _():
        send_waves(1)

    got = t_recv.at[0 : n - 1]
    remote(got, got, ts_sem, tr_sem, (x, y, z, c)).wait_recv()
    wait_waves(0)

    depth_all = n * lats
    pair_id = pair_smem[jnp.where(c == 0, x * n + z, z * n + y)]
    limit = TRUNC - SPACING * pair_id - SPACING // 2

    def turn_waves(u):
        for s in range(sides):
            w_turned[u, s * LANE : (s + 1) * LANE] = w_recv[u, :, s].reshape(depth_all, LANE).T

    def table_of(j0, j1):
        return t_recv[:, :, :, j0 * LANE : j1 * LANE].reshape(depth_all, (j1 - j0) * LANE)

    all_spans = [(k, min(k + 2, j1)) for j0, j1 in PIECES for k in range(j0, j1, 2)]

    def sums_of(u, k0, k1):
        sums = jnp.dot(w_turned[u], table_of(k0, k1), preferred_element_type=jnp.float32)
        return sums.reshape(n, 2 * ch, (k1 - k0) * LANE)

    turn_waves(0)
    for k0, k1 in all_spans:
        part[:, :, k0 * LANE : k1 * LANE] = sums_of(0, k0, k1)

    @pl.when(c == 1)
    def _():
        wait_waves(1)
        turn_waves(1)

    def product_high(j0, j1):
        @pl.when(c == 1)
        def _():
            for k0, k1 in all_spans:
                if j0 <= k0 < j1:
                    at = slice(k0 * LANE, k1 * LANE)
                    column = half + k0 * LANE + iota((n, 2 * ch, (k1 - k0) * LANE), 2)
                    part[:, :, at] = jnp.where(column < limit, part[:, :, at], sums_of(1, k0, k1))

    def up(k):
        return wrap(me_second + k)

    far = n == 8
    ways = ((1, -1), (0, 1)) if far else ((0, 1),)
    stage, near, late = {}, {}, {}

    def span_of(p):
        return slice(PIECES[p][0] * LANE, PIECES[p][1] * LANE)

    def send_far(p):
        at = span_of(p)
        for i, sign in ways if far else ():
            stage[p, i] = (
                remote(
                    part.at[up(3 * sign), :, at], a3.at[i, :, at], a_ssem.at[p, i], a_rsem.at[p, i],
                    second_axis(up(sign)),
                ),
                remote(
                    part.at[up(4), i * ch : (i + 1) * ch, at], a4.at[i, :, at], a_ssem.at[p, 2 + i],
                    a_rsem.at[p, 2 + i], second_axis(up(2 * sign)),
                ),
            )
            for send in stage[p, i]:
                send.start()

    def send_near(p):
        at = span_of(p)
        for i, sign in ways:
            near[p, i] = remote(
                part.at[up(sign), :, at], fin.at[i, :, at], f_ssem.at[p, i], f_rsem.at[p, i], second_axis(up(sign))
            )
            near[p, i].start()

    def merge(p):
        at = span_of(p)
        for i, sign in ways if far else ():
            stage[p, i][0].wait_recv()
            merged[i, :, at] = part[up(2 * sign), :, at] + a3[i, :, at]
            stage[p, i][1].wait_recv()
            mine = slice(i * ch, (i + 1) * ch)
            merged[i, mine, at] = merged[i, mine, at] + a4[i, :, at]
            late[p, i] = remote(
                merged.at[i, :, at], fin.at[2 + i, :, at], f_ssem.at[p, 2 + i], f_rsem.at[p, 2 + i],
                second_axis(up(2 * sign)),
            )
            late[p, i].start()

    def final(p):
        at = span_of(p)
        total = part[me_second, :, at]
        for i, _ in ways:
            near[p, i].wait_recv()
            total = total + fin[i, :, at]
        for i, _ in ways if far else ():
            late[p, i].wait_recv()
            total = total + fin[2 + i, :, at]
        return total

    product_high(*PIECES[0])
    send_far(0)
    product_high(*PIECES[1])
    send_far(1)
    send_near(0)
    merge(0)
    merge(1)
    send_near(1)
    total = jnp.concatenate([final(0), final(1)], axis=1)

    levels = sources * ch // 2
    channel = me_second * 2 * ch + iota((2 * ch, LANE), 0)
    factor = 1.0 + 2.0 * lax.shift_right_logical(channel, 1).astype(jnp.float32) / (levels - 1)
    squares = None
    for j in range(chunks):
        column = total[:, j * LANE : (j + 1) * LANE]
        squares = column * column if squares is None else squares + column * column
    squares = factor * squares
    tile = squares[0:8]
    for i in range(1, 2 * ch // 8):
        tile = tile + squares[i * 8 : i * 8 + 8]
    tile = jnp.sum(tile, axis=0, keepdims=True)

    def share(ref, at, tile, sem, devices):
        ref[at] = tile
        for device in devices:
            remote(ref.at[at], ref.at[at], e_ssem.at[sem], e_rsem.at[sem], device).start()

    def added(ref, size, sem):
        got = ref.at[0 : size - 1]
        remote(got, got, e_ssem.at[sem], e_rsem.at[sem], (x, y, z, c)).wait_recv()
        tile = ref[0]
        for i in range(1, size):
            tile = tile + ref[i]
        return tile

    peers = [(x, y, wrap(z + r), k) for r in far_first for k in (c, other)] + [(x, y, z, other)]
    share(e0, me, tile, 0, peers)
    total_ref[...] = total

    tile = added(e0, sources, 0)
    at_home = jnp.where(c == 0, y, x) == z

    def rows_of(core):
        return total_ref.at[pl.ds(pl.multiple_of(core * ch, 8), ch)]

    home = out_hbm.at[:, pl.ds(pl.multiple_of(c * half, LANE), half)]
    at_home_copy = pltpu.make_async_copy(rows_of(c), home, load_sem.at[5])

    def to_owner(core):
        device = (jnp.where(c == 0, x, z), jnp.where(c == 0, z, y), me_second, core)
        return remote(rows_of(core), home, o_ssem.at[core], o_rsem.at[c], device)

    ring = [min(r, n - r) for r in range(n)]
    steps = sorted(((i, j) for i in range(n) for j in range(n) if i or j), key=lambda s: -ring[s[0]] - ring[s[1]])
    e_row[...] = tile
    e_own = e1_hbm.at[x * n + y]
    def share_row(steps):
        for i, j in steps:
            remote(e_row, e_own, e_ssem.at[1], e_rsem.at[1], (wrap(x + i), wrap(y + j), z, c)).start()

    far_steps = len(steps) // 3
    share_row(steps[:far_steps])
    to_owner(other).start()

    @pl.when(at_home)
    def _():
        at_home_copy.start()

    @pl.when(jnp.logical_not(at_home))
    def _():
        to_owner(c).start()

    share_row(steps[far_steps:])
    e_copy = pltpu.make_async_copy(e_row, e_own, load_sem.at[6])
    e_copy.start()

    got = e1_hbm.at[0 : pairs - 1]
    remote(got, got, e_ssem.at[1], e_rsem.at[1], (x, y, z, c)).wait_recv()
    e_copy.wait()

    def from_core(core):
        got = out_hbm.at[:, pl.ds(pl.multiple_of(core * half, LANE), half)]
        return remote(got, got, o_ssem.at[core], o_rsem.at[core], (x, y, z, c))

    from_core(other).wait_recv()

    @pl.when(at_home)
    def _():
        at_home_copy.wait()

    @pl.when(jnp.logical_not(at_home))
    def _():
        from_core(c).wait_recv()

    first = z_recv.at[0, 0 : sources - 1]
    remote(first, first, zs_sem.at[0], zr_sem.at[0], (x, y, z, c)).wait_send()

    @pl.when(c == 0)
    def _():
        second = z_recv.at[1, 0:n]
        remote(second, second, zs_sem.at[1], zr_sem.at[1], (x, y, z, c)).wait_send()

    @pl.when(c == 1)
    def _():
        second = z_recv.at[1, 0 : n - 1]
        remote(second, second, zs_sem.at[1], zr_sem.at[1], (x, y, z, c)).wait_send()
        gone = w_send.at[1, 0 : n - 1]
        remote(gone, gone, ws_sem.at[1], wr_sem.at[1], (x, y, z, c)).wait_send()

    gone = w_send.at[0, 0 : n - 1]
    remote(gone, gone, ws_sem.at[0], wr_sem.at[0], (x, y, z, c)).wait_send()
    gone = t_send.at[0 : n - 1]
    remote(gone, gone, ts_sem, tr_sem, (x, y, z, c)).wait_send()
    for key in near:
        near[key].wait_send()
    for key in late:
        stage[key][0].wait_send()
        stage[key][1].wait_send()
        late[key].wait_send()
    to_owner(other).wait_send()

    @pl.when(jnp.logical_not(at_home))
    def _():
        to_owner(c).wait_send()

    for sem, ref, size in ((0, e0, sources), (1, e1_hbm, pairs)):
        gone = ref.at[0 : size - 1]
        remote(gone, gone, e_ssem.at[sem], e_rsem.at[sem], (x, y, z, c)).wait_send()


def outputs_kernel(scale, block_hbm, rows_hbm, out_hbm, energy_hbm, block, rows, energy, sem):
    loads = [pltpu.make_async_copy(rows_hbm, rows, sem.at[0]), pltpu.make_async_copy(block_hbm, block, sem.at[1])]
    stores = [pltpu.make_async_copy(energy, energy_hbm, sem.at[2]), pltpu.make_async_copy(block, out_hbm, sem.at[3])]
    for load in loads:
        load.start()
    loads[1].wait()
    stores[1].start()
    loads[0].wait()
    energy[0, 0] = jnp.sum(jnp.sum(rows[...], axis=0)) * scale
    stores[0].start()
    for store in stores:
        store.wait()


def shards(n, fourier, quad_weights, legendre, owner_pair):
    ch, lats, _ = fourier.shape
    _, pairs, length = legendre.shape
    half = length // 2
    rows = LANE // ch
    blocks = lats // rows
    sides = 2 * n // rows
    bf16, f32 = jnp.bfloat16, jnp.float32
    vmem, dma = pltpu.VMEM, pltpu.SemaphoreType.DMA
    hbm = pl.BlockSpec(memory_space=pltpu.HBM)
    limit = pltpu.CompilerParams(vmem_limit_bytes=67_043_328)
    block, energy_rows = pl.pallas_call(
        functools.partial(kernel, n),
        out_shape=(
            jax.ShapeDtypeStruct((ch, length), f32),
            jax.ShapeDtypeStruct((pairs, 1, LANE), f32),
        ),
        in_specs=[hbm] * 5,
        out_specs=(hbm, hbm),
        scratch_shapes=[
            vmem((ch, lats, M_WIN), bf16),
            vmem((ch * lats, M_WIN), f32),
            vmem((blocks, LANE, M_WIN), bf16),
            vmem((lats, pairs, half), bf16),
            vmem((1, pairs), jnp.int32),
            pltpu.SMEM((pairs,), jnp.int32),
            pltpu.SMEM((lats,), f32),
            vmem((3, n, blocks, n, LANE), bf16),
            vmem((2, 2 * n, blocks, n, LANE), bf16),
            vmem((2, n, sides, blocks, rows, LANE), bf16),
            vmem((2, n, sides, blocks, rows, LANE), bf16),
            vmem((2, 2 * n * ch, n * lats), bf16),
            vmem((n, blocks, rows, half), bf16),
            vmem((n, blocks, rows, half), bf16),
            vmem((n, 2 * ch, half), f32),
            vmem((2, 2 * ch, half), f32),
            vmem((2, ch, half), f32),
            vmem((2, 2 * ch, half), f32),
            vmem((4, 2 * ch, half), f32),
            vmem((2 * ch, half), f32),
            vmem((2 * n, 1, LANE), f32),
            vmem((1, LANE), f32),
            dma((7,)),
            dma((2,)),
            dma((2,)),
            dma((2,)),
            dma((2,)),
            dma,
            dma,
            dma((2, 4)),
            dma((2, 4)),
            dma((2, 4)),
            dma((2, 4)),
            dma((2,)),
            dma((2,)),
            dma((2,)),
            dma((2,)),
        ],
        compiler_params=pltpu.CompilerParams(collective_id=0, has_side_effects=True, vmem_limit_bytes=67_043_328),
        name="legendre",
    )(fourier, quad_weights, legendre, owner_pair.reshape(1, pairs), owner_pair)
    spectra, energy = pl.pallas_call(
        functools.partial(outputs_kernel, 1.0 / (pairs * 2 * n * ch * length)),
        out_shape=(
            jax.ShapeDtypeStruct((ch, length), f32),
            jax.ShapeDtypeStruct((1, 1), f32),
        ),
        in_specs=[hbm] * 2,
        out_specs=(hbm, hbm),
        scratch_shapes=[vmem((ch, length), f32), vmem((pairs, 1, LANE), f32), pltpu.SMEM((1, 1), f32), dma((4,))],
        compiler_params=limit,
        name="outputs",
    )(block, energy_rows)
    return spectra[None], energy[0, 0]


def solution(mesh):
    n = mesh.shape["lev"] // 2
    finer = Mesh(mesh.devices.reshape(n, n, n, 2), LAT + LEV)
    return jax.shard_map(
        functools.partial(shards, n),
        mesh=finer,
        in_specs=(P(LEV, LAT, None), P(LAT), P(LAT, None, None), P()),
        out_specs=(P(LAT, LEV, None), P()),
        check_vma=False,
    )
```
